64 devices in a mesh: dp: 4 (over x, y), cp: 16 (over z, core).
Axes of the slice: x: 2, y: 2, z: 8, core: 2. Of those that a mesh axis runs over, the one named last changes fastest.
The devices are a block of a 4x4x8 slice.
Arguments:
- x: bfloat16 [32, 5120], P('dp'), parts along dimension 0
- w_dq: bfloat16 [5120, 1536], replicated
- g_q: float32 [1536], replicated
- w_uq: bfloat16 [1536, 24576], replicated
- w_dkv: bfloat16 [5120, 576], replicated
- g_kv: float32 [512], replicated
- w_uk: bfloat16 [512, 128, 128], replicated
- w_uv: bfloat16 [512, 128, 128], replicated
- w_o: bfloat16 [16384, 5120], replicated
- cache_c: bfloat16 [32, 32768, 512], P('dp', 'cp'), parts along dimension 0
- cache_kr: bfloat16 [32, 32768, 64], P('dp', 'cp'), parts along dimension 0
- ctx_len: int32 [32], P('dp'), parts along dimension 0
Outputs:
- output 1: bfloat16 [32, 5120], P('dp'), parts along dimension 0
- output 2: bfloat16 [32, 512], P('dp'), parts along dimension 0
- output 3: bfloat16 [32, 64], P('dp'), parts along dimension 0
There are 4 independent parts. The reference program is written for one: setup_inputs(seed, part) draws one part's arguments, and reference() takes and returns one part's arrays. A program takes and returns all parts, laid end to end along the dimension named above; an argument that names none is the same for every part.
All inputs are finite; a program needn't handle non-finite values.
Results may differ from the reference program's by a relative error of at most 0.00631236.
Values sent between devices are 32-bit elements.
A program may use at most 768 MiB of HBM per device.

```python
import jax
import jax.numpy as jnp
from jax import lax

BATCH = 8
T_DEV = 2048
GROUP_SIZE = 16
D_MODEL = 5120
HEADS = 128
Q_LORA = 1536
LATENT = 512
NOPE_DIM = 128
ROPE_DIM = 64
V_DIM = 128

SEQ = T_DEV * GROUP_SIZE
QK_DIM = NOPE_DIM + ROPE_DIM
NORM_EPS = 1e-6
ROPE_THETA = 10000.0


def rms_norm(values, gain_vec):
    mean_sq = jnp.mean(jnp.square(values), axis=-1, keepdims=True)
    return values * lax.rsqrt(mean_sq + NORM_EPS) * gain_vec


def rope_tables(positions):
    half_dim = ROPE_DIM // 2
    inv_freq = ROPE_THETA ** (-2.0 * jnp.arange(half_dim, dtype=jnp.float32) / ROPE_DIM)
    angles = positions.astype(jnp.float32)[..., None] * inv_freq
    return jnp.cos(angles), jnp.sin(angles)


def rope_rotate(values, cos_tab, sin_tab):
    half_dim = values.shape[-1] // 2
    lo_half = values[..., :half_dim]
    hi_half = values[..., half_dim:]
    return jnp.concatenate([lo_half * cos_tab - hi_half * sin_tab, hi_half * cos_tab + lo_half * sin_tab], axis=-1)


def setup_inputs(seed: int = 0, part: int = 0) -> dict:
    shared_keys = jax.random.split(jax.random.key(seed), 8)
    part_keys = jax.random.split(jax.random.fold_in(jax.random.key(seed + 1), part), 8)

    def draw_normal(key, shape, std):
        return jax.random.normal(key, shape, jnp.float32) * std

    x = draw_normal(part_keys[0], (BATCH, D_MODEL), 1.0).astype(jnp.bfloat16)
    w_dq = draw_normal(shared_keys[0], (D_MODEL, Q_LORA), D_MODEL ** -0.5).astype(jnp.bfloat16)
    g_q = jax.random.uniform(shared_keys[1], (Q_LORA,), jnp.float32, 0.5, 1.5)
    w_uq = draw_normal(shared_keys[2], (Q_LORA, HEADS * QK_DIM), Q_LORA ** -0.5).astype(jnp.bfloat16)
    w_dkv = draw_normal(shared_keys[3], (D_MODEL, LATENT + ROPE_DIM), D_MODEL ** -0.5).astype(jnp.bfloat16)
    g_kv = jax.random.uniform(shared_keys[4], (LATENT,), jnp.float32, 0.5, 1.5)
    w_uk = draw_normal(shared_keys[5], (LATENT, HEADS, NOPE_DIM), LATENT ** -0.5).astype(jnp.bfloat16)
    w_uv = draw_normal(shared_keys[6], (LATENT, HEADS, V_DIM), LATENT ** -0.5).astype(jnp.bfloat16)
    w_o = draw_normal(shared_keys[7], (HEADS * V_DIM, D_MODEL), (HEADS * V_DIM) ** -0.5).astype(jnp.bfloat16)
    pos_ramp = 2.0 * jnp.arange(SEQ, dtype=jnp.float32) / SEQ - 1.0
    drift_dir = draw_normal(part_keys[1], (BATCH, 1, LATENT), 1.0)
    cache_c = (draw_normal(part_keys[2], (BATCH, SEQ, LATENT), 1.0) + drift_dir * pos_ramp[None, :, None]).astype(jnp.bfloat16)
    key_base = jnp.broadcast_to(draw_normal(part_keys[3], (BATCH, 1, ROPE_DIM), 1.0), (BATCH, SEQ, ROPE_DIM))
    cos_tab, sin_tab = rope_tables(jnp.arange(SEQ))
    cache_kr = (rope_rotate(key_base, cos_tab[None], sin_tab[None]) + draw_normal(part_keys[4], (BATCH, SEQ, ROPE_DIM), 0.5)).astype(jnp.bfloat16)
    ctx_len = jax.random.randint(part_keys[5], (BATCH,), SEQ // 2, SEQ, dtype=jnp.int32).at[0].set(SEQ - 1)
    return {'x': x, 'w_dq': w_dq, 'g_q': g_q, 'w_uq': w_uq, 'w_dkv': w_dkv, 'g_kv': g_kv, 'w_uk': w_uk, 'w_uv': w_uv, 'w_o': w_o, 'cache_c': cache_c, 'cache_kr': cache_kr, 'ctx_len': ctx_len}


def reference(x, w_dq, g_q, w_uq, w_dkv, g_kv, w_uk, w_uv, w_o, cache_c, cache_kr, ctx_len):
    cq_low = jnp.dot(x, w_dq, preferred_element_type=jnp.float32).astype(jnp.bfloat16)
    cq_norm = rms_norm(cq_low.astype(jnp.float32), g_q).astype(jnp.bfloat16)
    q_full = jnp.dot(cq_norm, w_uq, preferred_element_type=jnp.float32).astype(jnp.bfloat16).reshape(BATCH, HEADS, QK_DIM)
    cos_tab, sin_tab = rope_tables(ctx_len)
    q_rope = rope_rotate(q_full[:, :, NOPE_DIM:].astype(jnp.float32), cos_tab[:, None, :], sin_tab[:, None, :]).astype(jnp.bfloat16)
    q_lat = jnp.einsum('bhn,khn->bhk', q_full[:, :, :NOPE_DIM].astype(jnp.float32), w_uk.astype(jnp.float32)).astype(jnp.bfloat16)
    kv_full = jnp.dot(x, w_dkv, preferred_element_type=jnp.float32)
    c_new = rms_norm(kv_full[:, :LATENT], g_kv).astype(jnp.bfloat16)
    kr_new = rope_rotate(kv_full[:, LATENT:], cos_tab, sin_tab).astype(jnp.bfloat16)
    score_scale = QK_DIM ** -0.5
    positions = jnp.arange(SEQ)

    def attend_one(item_args):
        q_lat_r, q_rope_r, c_rows, kr_rows, c_new_r, kr_new_r, req_len = item_args
        scores = (jnp.dot(q_lat_r, c_rows.T, preferred_element_type=jnp.float32) + jnp.dot(q_rope_r, kr_rows.T, preferred_element_type=jnp.float32)) * score_scale
        scores = jnp.where(positions[None, :] < req_len, scores, -jnp.inf)
        new_score = (jnp.dot(q_lat_r, c_new_r, preferred_element_type=jnp.float32) + jnp.dot(q_rope_r, kr_new_r, preferred_element_type=jnp.float32)) * score_scale
        row_max = jnp.maximum(jnp.max(scores, axis=1), new_score)
        weights = jnp.exp(scores - row_max[:, None])
        new_weight = jnp.exp(new_score - row_max)
        row_sum = jnp.sum(weights, axis=1) + new_weight
        lat_acc = jnp.dot(weights.astype(jnp.bfloat16), c_rows, preferred_element_type=jnp.float32)
        lat_acc = lat_acc + new_weight.astype(jnp.bfloat16).astype(jnp.float32)[:, None] * c_new_r.astype(jnp.float32)[None, :]
        return lat_acc / row_sum[:, None]

    o_lat = lax.map(attend_one, (q_lat, q_rope, cache_c, cache_kr, c_new, kr_new, ctx_len)).astype(jnp.bfloat16)
    o_heads = jnp.einsum('bhk,khv->bhv', o_lat.astype(jnp.float32), w_uv.astype(jnp.float32)).astype(jnp.bfloat16)
    attn_out = jnp.dot(o_heads.reshape(BATCH, HEADS * V_DIM), w_o, preferred_element_type=jnp.float32)
    x_out = (x.astype(jnp.float32) + attn_out).astype(jnp.bfloat16)
    return x_out, c_new, kr_new
```

```python
import functools

import jax
import jax.numpy as jnp
from jax import lax
from jax.experimental import pallas as pl
from jax.experimental.pallas import tpu as pltpu
from jax.sharding import PartitionSpec as P

NORM_EPS = 1e-6
ROPE_THETA = 10000.0
LANES = 128
LOWEST = float(jnp.finfo(jnp.float32).min)
MESH = pl.DeviceIdType.MESH


def rms_norm(values, gain_vec):
    mean_sq = jnp.mean(jnp.square(values), axis=-1, keepdims=True)
    return values * lax.rsqrt(mean_sq + NORM_EPS) * gain_vec


def rope_tables(positions, rope_dim):
    half_dim = rope_dim // 2
    inv_freq = ROPE_THETA ** (-2.0 * jnp.arange(half_dim, dtype=jnp.float32) / rope_dim)
    angles = positions.astype(jnp.float32)[..., None] * inv_freq
    return jnp.cos(angles), jnp.sin(angles)


def rope_rotate(values, cos_tab, sin_tab):
    half_dim = values.shape[-1] // 2
    lo_half = values[..., :half_dim]
    hi_half = values[..., half_dim:]
    return jnp.concatenate([lo_half * cos_tab - hi_half * sin_tab, hi_half * cos_tab + lo_half * sin_tab], axis=-1)


def latent_step(x, w_dq, g_q, w_dkv, g_kv, ctx_len):
    latent = g_kv.shape[0]
    rope_dim = w_dkv.shape[1] - latent
    cq_low = jnp.dot(x, w_dq, preferred_element_type=jnp.float32).astype(jnp.bfloat16)
    cq_norm = rms_norm(cq_low.astype(jnp.float32), g_q).astype(jnp.bfloat16)
    cos_tab, sin_tab = rope_tables(ctx_len, rope_dim)
    kv_full = jnp.dot(x, w_dkv, preferred_element_type=jnp.float32)
    c_new = rms_norm(kv_full[:, :latent], g_kv).astype(jnp.bfloat16)
    kr_new = rope_rotate(kv_full[:, latent:], cos_tab, sin_tab).astype(jnp.bfloat16)
    return cq_norm, cos_tab, sin_tab, c_new, kr_new


def head_queries(cq_norm, w_uq, w_uk, cos_tab, sin_tab):
    n_req = cq_norm.shape[0]
    n_heads, nope_dim = w_uk.shape[1:]
    q_full = jnp.dot(cq_norm, w_uq, preferred_element_type=jnp.float32).astype(jnp.bfloat16)
    q_full = q_full.reshape(n_req, n_heads, -1)
    q_rope = rope_rotate(q_full[:, :, nope_dim:].astype(jnp.float32), cos_tab[:, None, :], sin_tab[:, None, :])
    q_lat = jnp.einsum('bhn,khn->bhk', q_full[:, :, :nope_dim], w_uk, preferred_element_type=jnp.float32)
    return q_lat.astype(jnp.bfloat16), q_rope.astype(jnp.bfloat16)


def merge(left, right, latent):
    half = LANES // 2
    m_l, m_r = left[:, latent:latent + 1], right[:, latent:latent + 1]
    l_l, l_r = left[:, latent + half:latent + half + 1], right[:, latent + half:latent + half + 1]
    top = jnp.maximum(m_l, m_r)
    f_l, f_r = jnp.exp(m_l - top), jnp.exp(m_r - top)
    acc = left[:, :latent] * f_l + right[:, :latent] * f_r
    return acc, top, l_l * f_l + l_r * f_r


def put_block(ref, index, acc, top, mass):
    latent = acc.shape[-1]
    rows = acc.shape[0]
    shape = ref.at[index].shape
    half = LANES // 2
    ref[index + (slice(None),) * (len(shape) - 1) + (slice(0, latent),)] = acc.reshape(shape[:-1] + (latent,))
    stats = jnp.where(lax.broadcasted_iota(jnp.int32, (rows, LANES), 1) < half, top, mass)
    ref[index + (slice(None),) * (len(shape) - 1) + (slice(latent, latent + LANES),)] = stats.reshape(shape[:-1] + (LANES,))


def attend_kernel(nz, scale, ctx_ref, q_ref, cn_ref, kn_ref, c_hbm, k_hbm, out_ref,
                  c_buf, k_buf, q_all, s_buf, own, other, mine, chain, hop_out,
                  c_sem, k_sem, q_recv, q_send, q_send_x, x_send, x_recv, h_send, h_recv):
    n_req, t_dev, latent = c_buf.shape
    rope_dim = k_buf.shape[1]
    per = q_ref.shape[1]
    n_dev = 2 * nz
    heads = n_dev * per
    far = nz // 2
    me = lax.axis_index('cp')
    z, core = me // 2, me % 2
    partner = me + 1 - 2 * core
    at = lambda off: lax.rem(z + off + nz, nz)
    sides = (at(1) * 2 + core, at(-1) * 2 + core)
    hops_from = (lambda off: at(-off) * 2 + core, lambda off: at(off) * 2 + core)

    def remote(src, dst, send, recv, target):
        return pltpu.make_async_remote_copy(src_ref=src, dst_ref=dst, send_sem=send, recv_sem=recv,
                                            device_id={'cp': target}, device_id_type=MESH)

    for r in range(n_req):
        pltpu.make_async_copy(c_hbm.at[r], c_buf.at[r], c_sem.at[r]).start()
        pltpu.make_async_copy(k_hbm.at[r], k_buf.at[r], k_sem.at[r]).start()

    barrier = pltpu.get_barrier_semaphore()
    for peer in (*sides, partner):
        pl.semaphore_signal(barrier, inc=1, device_id={'cp': peer}, device_id_type=MESH)
    q_all[:, pl.ds(me, 1)] = q_ref[...].reshape(n_req, 1, per, latent + LANES)
    pl.semaphore_wait(barrier, 3)

    def ring_copy(r, hop, way, src_dev):
        src = q_ref.at[r] if hop == 1 else q_all.at[r, src_dev]
        return remote(src, q_all.at[r, src_dev], q_send.at[r, hop - 1, way], q_recv.at[r, src_dev], sides[way])

    def cross_copy(r, slot, src_dev):
        src = q_ref.at[r] if slot == 0 else q_all.at[r, src_dev]
        return remote(src, q_all.at[r, src_dev], q_send_x.at[r, slot], q_recv.at[r, src_dev], partner)

    def arrived(r, src_dev):
        remote(q_all.at[r, src_dev], q_all.at[r, src_dev], q_send.at[r, 0, 0], q_recv.at[r, src_dev], partner).wait_recv()

    def gather_hop(r, hop):
        if hop == 1:
            for way in range(2):
                ring_copy(r, hop, way, me).start()
            cross_copy(r, 0, me).start()
            return
        for way in range(2):
            src_dev = hops_from[way](hop - 1)

            def forward(way=way, src_dev=src_dev):
                arrived(r, src_dev)
                if hop <= far:
                    if hop == far:
                        @pl.when(core == way)
                        def _():
                            ring_copy(r, hop, way, src_dev).start()
                    else:
                        ring_copy(r, hop, way, src_dev).start()
                cross_copy(r, 2 * (hop - 2) + way + 1 if hop <= far else 2 * far - 1, src_dev).start()

            if hop == far + 1:
                pl.when(core == way)(forward)
            else:
                forward()

    def attend(r):
        def from_partner(d, carry):
            arrived(r, d * 2 + 1 - core)
            return carry
        lax.fori_loop(0, nz, from_partner, 0)
        pltpu.make_async_copy(c_hbm.at[r], c_buf.at[r], c_sem.at[r]).wait()
        pltpu.make_async_copy(k_hbm.at[r], k_buf.at[r], k_sem.at[r]).wait()
        q = q_all[r].reshape(heads, latent + LANES)
        q_lat = q[:, :latent].astype(jnp.bfloat16)
        q_rope = q[:, latent:latent + rope_dim].astype(jnp.bfloat16)
        n = ctx_ref[r]
        base = me * t_dev
        step = 512
        top = jnp.full((heads, LANES), LOWEST, jnp.float32)

        def valid(t0):
            return base + t0 + lax.broadcasted_iota(jnp.int32, (1, step), 1) < n

        for t0 in range(0, t_dev, step):
            s = lax.dot_general(q_lat, c_buf[r, t0:t0 + step, :], (((1,), (1,)), ((), ())), preferred_element_type=jnp.float32)
            s += jnp.dot(q_rope, k_buf[r, :, t0:t0 + step], preferred_element_type=jnp.float32)
            s = jnp.where(valid(t0), s * scale, LOWEST)
            s_buf[:, t0:t0 + step] = s
            for j in range(0, step, LANES):
                top = jnp.maximum(top, s[:, j:j + LANES])
        c_new = cn_ref[r]
        kr_new = kn_ref[r]
        s_new = (jnp.sum(q_lat.astype(jnp.float32) * c_new, axis=1, keepdims=True)
                 + jnp.sum(q_rope.astype(jnp.float32) * kr_new, axis=1, keepdims=True)) * scale
        owner = jnp.logical_and(n >= base, n < base + t_dev)
        s_new = jnp.where(owner, s_new, LOWEST)
        m = jnp.maximum(jnp.max(top, axis=1, keepdims=True), s_new)
        w_new = jnp.where(owner, jnp.exp(s_new - m), 0.0)
        mass = jnp.zeros((heads, LANES), jnp.float32)
        acc = w_new.astype(jnp.bfloat16).astype(jnp.float32) * c_new
        for t0 in range(0, t_dev, step):
            w = jnp.where(valid(t0), jnp.exp(s_buf[:, t0:t0 + step] - m), 0.0)
            for j in range(0, step, LANES):
                mass += w[:, j:j + LANES]
            acc += jnp.dot(w.astype(jnp.bfloat16), c_buf[r, t0:t0 + step, :], preferred_element_type=jnp.float32)
        put_block(own, (r,), acc, m, jnp.sum(mass, axis=1, keepdims=True) + w_new)

    def cross_sum(r):
        return remote(own.at[r, :, 1 - core], other.at[r], x_send.at[r], x_recv.at[r], partner)

    def chain_copy(r, hop, way, src):
        return remote(src, chain.at[r, hop - 1, way], h_send.at[r, hop - 1, way], h_recv.at[r, hop - 1, way], sides[way])

    def flat(block):
        return block.reshape(-1, latent + LANES)

    def reduce_hop(r, hop):
        if hop == 1:
            cross_sum(r).wait_recv()
            put_block(mine, (r,), *merge(flat(own[r, :, core]), flat(other[r]), latent))
        for way in range(2):
            dest = at((far + 1 - hop) * (1 - 2 * way))
            if hop == 1:
                @pl.when(core == way)
                def _(way=way, dest=dest):
                    chain_copy(r, hop, way, mine.at[r, dest]).start()
                continue

            def pass_on(way=way, dest=dest):
                chain_copy(r, hop - 1, way, chain.at[r, hop - 2, way]).wait_recv()
                put_block(hop_out, (r, hop - 2, way), *merge(chain[r, hop - 2, way], mine[r, dest], latent))
                chain_copy(r, hop, way, hop_out.at[r, hop - 2, way]).start()

            if hop == 2:
                pl.when(core == way)(pass_on)

                @pl.when(core != way)
                def _(way=way, dest=dest):
                    chain_copy(r, hop, way, mine.at[r, dest]).start()
            else:
                pass_on()

    def finish(r):
        for way in range(2):
            chain_copy(r, far, way, chain.at[r, far - 1, way]).wait_recv()
        acc, top, mass = merge(chain[r, far - 1, 0], chain[r, far - 1, 1], latent)
        stats = jnp.where(lax.broadcasted_iota(jnp.int32, (per, LANES), 1) < LANES // 2, top, mass)
        both = jnp.concatenate([acc, stats], axis=1)
        acc, top, mass = merge(both, mine[r, z], latent)
        out_ref[r] = (acc / mass).astype(out_ref.dtype)

    def slot(s, carry):
        def at_slot(delay, body):
            r = s - delay

            @pl.when(jnp.logical_and(r >= 0, r < n_req))
            def _():
                body(r)

        for hop in range(far + 1, 0, -1):
            at_slot(hop - 1, functools.partial(gather_hop, hop=hop))
        at_slot(2 * far + 2, finish)
        for hop in range(far, 0, -1):
            at_slot(far + 1 + hop, functools.partial(reduce_hop, hop=hop))

        def compute(r):
            attend(r)
            cross_sum(r).start()
        at_slot(far + 1, compute)
        return carry

    lax.fori_loop(0, n_req + 2 * far + 2, slot, 0)

    def drain(r, carry):
        for way in range(2):
            for hop in range(1, far + 1):
                def ring_done(way=way, hop=hop):
                    ring_copy(r, hop, way, me).wait_send()

                def chain_done(way=way, hop=hop):
                    chain_copy(r, hop, way, mine.at[r, 0]).wait_send()
                pl.when(core == way)(ring_done) if hop == far else ring_done()
                pl.when(core == way)(chain_done) if hop == 1 else chain_done()
        for slot_x in range(nz):
            cross_copy(r, slot_x, me).wait_send()
        cross_sum(r).wait_send()
        return carry
    lax.fori_loop(0, n_req, drain, 0)


def attend_blocks(nz, ctx_len, q_own, c_new, kr_new, cache_c, cache_krt, scale):
    n_req, per, width = q_own.shape
    _, t_dev, latent = cache_c.shape
    rope_dim = cache_krt.shape[1]
    far = nz // 2
    heads = 2 * nz * per
    vmem = pl.BlockSpec(memory_space=pltpu.VMEM)
    hbm = pl.BlockSpec(memory_space=pl.ANY)
    dma = pltpu.SemaphoreType.DMA
    f32 = jnp.float32
    return pl.pallas_call(
        functools.partial(attend_kernel, nz, scale),
        out_shape=jax.ShapeDtypeStruct((n_req, per, latent), jnp.bfloat16),
        in_specs=[pl.BlockSpec(memory_space=pltpu.SMEM), vmem, vmem, vmem, hbm, hbm],
        out_specs=vmem,
        scratch_shapes=[
            pltpu.VMEM((n_req, t_dev, latent), jnp.bfloat16),
            pltpu.VMEM((n_req, rope_dim, t_dev), jnp.bfloat16),
            pltpu.VMEM((n_req, 2 * nz, per, width), f32),
            pltpu.VMEM((heads, t_dev), f32),
            pltpu.VMEM((n_req, nz, 2, per, width), f32),
            pltpu.VMEM((n_req, nz, per, width), f32),
            pltpu.VMEM((n_req, nz, per, width), f32),
            pltpu.VMEM((n_req, far, 2, per, width), f32),
            pltpu.VMEM((n_req, far - 1, 2, per, width), f32),
            dma((n_req,)),
            dma((n_req,)),
            dma((n_req, 2 * nz)),
            dma((n_req, far, 2)),
            dma((n_req, nz)),
            dma((n_req,)),
            dma((n_req,)),
            dma((n_req, far, 2)),
            dma((n_req, far, 2)),
        ],
        compiler_params=pltpu.CompilerParams(collective_id=0, has_side_effects=True, vmem_limit_bytes=56 * 2 ** 20),
        name='attend_blocks',
    )(ctx_len, q_own, c_new, kr_new, cache_c, cache_krt)


def add_up_kernel(nz, part_ref, x_ref, out_ref, got, mine, theirs, total, a_send, a_recv, x_send, x_recv, b_send, b_recv):
    me = lax.axis_index('cp')
    z, core = me // 2, me % 2
    partner = me + 1 - 2 * core
    width = mine.shape[1]
    at = lambda off: lax.rem(z + off, nz)
    cols = lambda piece: pl.ds(pl.multiple_of(piece * width, LANES), width)

    def remote(src, dst, send, recv, target):
        return pltpu.make_async_remote_copy(src_ref=src, dst_ref=dst, send_sem=send, recv_sem=recv,
                                            device_id={'cp': target}, device_id_type=MESH)

    barrier = pltpu.get_barrier_semaphore()
    for off in range(1, nz):
        pl.semaphore_signal(barrier, inc=1, device_id={'cp': at(off) * 2 + core}, device_id_type=MESH)
    pl.semaphore_signal(barrier, inc=1, device_id={'cp': partner}, device_id_type=MESH)
    pl.semaphore_wait(barrier, nz)
    order = sorted(range(1, nz), key=lambda off: -min(off, nz - off))
    scatter = {off: remote(part_ref.at[:, cols(at(off))], got.at[off - 1], a_send.at[off - 1], a_recv.at[off - 1], at(off) * 2 + core) for off in order}
    for off in order:
        scatter[off].start()
    acc = part_ref[:, cols(z)]
    for off in reversed(order):
        scatter[off].wait_recv()
        acc += got[off - 1]
    mine[...] = acc
    swap = remote(mine, theirs, x_send, x_recv, partner)
    swap.start()
    swap.wait_recv()
    total[z] = mine[...] + theirs[...]
    spread = {off: remote(total.at[z], total.at[z], b_send.at[off - 1], b_recv.at[off - 1], at(off) * 2 + core) for off in order}
    for off in order:
        spread[off].start()
    for off in reversed(order):
        src = at(nz - off)
        remote(total.at[src], total.at[src], b_send.at[off - 1], b_recv.at[off - 1], at(off) * 2 + core).wait_recv()
    for piece in range(nz):
        span = slice(piece * width, (piece + 1) * width)
        out_ref[:, span] = (x_ref[:, span].astype(jnp.float32) + total[piece]).astype(out_ref.dtype)
    swap.wait_send()
    for off in order:
        scatter[off].wait_send()
        spread[off].wait_send()


def add_up(nz, part, x):
    rows, columns = part.shape
    width = columns // nz
    vmem = pl.BlockSpec(memory_space=pltpu.VMEM)
    dma = pltpu.SemaphoreType.DMA
    return pl.pallas_call(
        functools.partial(add_up_kernel, nz),
        out_shape=jax.ShapeDtypeStruct((rows, columns), x.dtype),
        in_specs=[vmem, vmem],
        out_specs=vmem,
        scratch_shapes=[
            pltpu.VMEM((nz - 1, rows, width), jnp.float32),
            pltpu.VMEM((rows, width), jnp.float32),
            pltpu.VMEM((rows, width), jnp.float32),
            pltpu.VMEM((nz, rows, width), jnp.float32),
            dma((nz - 1,)), dma((nz - 1,)), dma, dma, dma((nz - 1,)), dma((nz - 1,)),
        ],
        compiler_params=pltpu.CompilerParams(collective_id=1, has_side_effects=True),
        name='add_up',
    )(part, x)


def solution(mesh):
    n_cp = mesh.shape['cp']
    nz = n_cp // 2

    def decode_step(x, w_dq, g_q, w_uq, w_dkv, g_kv, w_uk, w_uv, w_o, cache_c, cache_kr, ctx_len):
        latent, n_heads, nope_dim = w_uk.shape
        n_req = x.shape[0]
        rope_dim = cache_kr.shape[2]
        per = n_heads // n_cp
        scale = (nope_dim + rope_dim) ** -0.5
        shard_idx = lax.axis_index('cp')
        cut = lambda w, axis, size: lax.dynamic_slice_in_dim(w, shard_idx * size, size, axis)
        cq_norm, cos_tab, sin_tab, c_new, kr_new = latent_step(x, w_dq, g_q, w_dkv, g_kv, ctx_len)
        q_lat, q_rope = head_queries(cq_norm, cut(w_uq, 1, per * (nope_dim + rope_dim)), cut(w_uk, 1, per), cos_tab, sin_tab)
        pad = jnp.zeros((n_req, per, LANES - rope_dim), jnp.float32)
        q_own = jnp.concatenate([q_lat.astype(jnp.float32), q_rope.astype(jnp.float32), pad], axis=2)
        o_lat = attend_blocks(nz, ctx_len, q_own, c_new.astype(jnp.float32)[:, None], kr_new.astype(jnp.float32)[:, None],
                              cache_c, cache_kr.transpose(0, 2, 1), scale)
        o_heads = jnp.einsum('bhk,khv->bhv', o_lat, cut(w_uv, 1, per), preferred_element_type=jnp.float32).astype(jnp.bfloat16)
        part = jnp.dot(o_heads.reshape(n_req, -1), cut(w_o, 0, per * w_uv.shape[2]), preferred_element_type=jnp.float32)
        return add_up(nz, part, x), c_new, kr_new

    spec_rows = P('dp', None)
    spec_cache = P('dp', 'cp', None)
    in_specs = (spec_rows, P(), P(), P(), P(), P(), P(), P(), P(), spec_cache, spec_cache, P('dp'))
    out_specs = (spec_rows, spec_rows, spec_rows)
    return jax.shard_map(decode_step, mesh=mesh, in_specs=in_specs, out_specs=out_specs, check_vma=False)
```

```python
import functools

import jax
import jax.numpy as jnp
from jax import lax
from jax.experimental import pallas as pl
from jax.experimental.pallas import tpu as pltpu
from jax.sharding import PartitionSpec as P

NORM_EPS = 1e-6
ROPE_THETA = 10000.0
LANES = 128
RELAY_TURN = 2
FAR_TURN = 4
LOWEST = float(jnp.finfo(jnp.float32).min)
MESH = pl.DeviceIdType.MESH


def rms_norm(values, gain_vec):
    mean_sq = jnp.mean(jnp.square(values), axis=-1, keepdims=True)
    return values * lax.rsqrt(mean_sq + NORM_EPS) * gain_vec


def rope_tables(positions, rope_dim):
    half_dim = rope_dim // 2
    inv_freq = ROPE_THETA ** (-2.0 * jnp.arange(half_dim, dtype=jnp.float32) / rope_dim)
    angles = positions.astype(jnp.float32)[..., None] * inv_freq
    return jnp.cos(angles), jnp.sin(angles)


def rope_rotate(values, cos_tab, sin_tab):
    half_dim = values.shape[-1] // 2
    swapped = jnp.concatenate([values[:, half_dim:], values[:, :half_dim]], axis=-1)
    return values * cos_tab + swapped * sin_tab


def merge(blocks, latent):
    half = LANES // 2
    tops = [block[:, latent:latent + 1] for block in blocks]
    top = functools.reduce(jnp.maximum, tops)
    factors = [jnp.exp(one - top) for one in tops]
    acc = sum(block[:, :latent] * factor for block, factor in zip(blocks, factors))
    mass = sum(block[:, latent + half:latent + half + 1] * factor for block, factor in zip(blocks, factors))
    return acc, top, mass


def put_block(ref, index, acc, top, mass):
    latent = acc.shape[-1]
    rows = acc.shape[0]
    shape = ref.at[index].shape
    half = LANES // 2
    ref[index + (slice(None),) * (len(shape) - 1) + (slice(0, latent),)] = acc.reshape(shape[:-1] + (latent,))
    stats = jnp.where(lax.broadcasted_iota(jnp.int32, (rows, LANES), 1) < half, top, mass)
    ref[index + (slice(None),) * (len(shape) - 1) + (slice(latent, latent + LANES),)] = stats.reshape(shape[:-1] + (LANES,))


def decode_kernel(nz, scale, ctx_ref, x_ref, gq_ref, gkv_ref, cos_ref, sin_ref,
                  wdq_hbm, wuq_hbm, wdkv_hbm, wuk_hbm, wuv_hbm, wo_hbm, c_hbm, k_hbm, out_ref, cnew_ref, knew_ref,
                  c_buf, k_buf, q_all, s_buf, own, other, mine, held, relay, last,
                  big, wuq_buf, wdkv_buf, uk_buf, uv_buf, wide, uk_heads, uv_heads,
                  cq_half, q_ref, cn_ref, kn_ref, o_lat, part, got, pair,
                  c_sem, k_sem, q_recv, q_send, q_send_x, x_send, x_recv, h_send, h_recv, f_send, f_recv,
                  w_sem, s_sem, r_sem, a_send, a_recv, b_send, b_recv):
    n_req, t_dev, latent = c_buf.shape
    rope_dim = k_buf.shape[1]
    per = q_ref.shape[1]
    q_half = cq_half.shape[2]
    v_dim = uv_heads.shape[2]
    nope_dim = uk_heads.shape[2]
    width = part.shape[2]
    n_dev = 2 * nz
    heads = n_dev * per
    me = lax.axis_index('cp')
    z, core = me // 2, me % 2
    partner = me + 1 - 2 * core
    at = lambda off: lax.rem(z + off + nz, nz)
    chip = lambda off: at(off) * 2 + core

    def remote(src, dst, send, recv, target):
        return pltpu.make_async_remote_copy(src_ref=src, dst_ref=dst, send_sem=send, recv_sem=recv,
                                            device_id={'cp': target}, device_id_type=MESH)

    rows = big.shape[0]
    head0 = pl.multiple_of(me * per, 8)
    weights = [pltpu.make_async_copy(wuk_hbm.at[:, pl.ds(head0, per)], uk_buf, w_sem.at[0])]
    q_cols = pl.ds(pl.multiple_of(core * q_half, LANES), q_half)
    blocks = x_ref.shape[1] // rows
    for i in range(blocks):
        weights.append(pltpu.make_async_copy(wdq_hbm.at[i * rows:(i + 1) * rows, q_cols], big.at[:, i * q_half:(i + 1) * q_half], w_sem.at[4 + i]))
    uq_cols = wuq_buf.shape[1]
    weights.append(pltpu.make_async_copy(wuq_hbm.at[:, pl.ds(pl.multiple_of(me * uq_cols, LANES), uq_cols)], wuq_buf, w_sem.at[1]))
    weights.append(pltpu.make_async_copy(wdkv_hbm, wdkv_buf, w_sem.at[2]))
    weights.append(pltpu.make_async_copy(wuv_hbm.at[:, pl.ds(head0, per)], uv_buf, w_sem.at[3]))
    for copy in weights:
        copy.start()
    for r in range(n_req):
        pltpu.make_async_copy(c_hbm.at[r], c_buf.at[r], c_sem.at[r]).start()
        pltpu.make_async_copy(k_hbm.at[r], k_buf.at[r], k_sem.at[r]).start()
    wait_uk, *wait_dq, wait_uq, wait_dkv, wait_uv = weights
    wo_copy = pltpu.make_async_copy(wo_hbm.at[pl.ds(pl.multiple_of(me * rows, LANES), rows)], big, w_sem.at[4])

    barrier = pltpu.get_barrier_semaphore()
    for peer in (*(chip(off) for off in range(1, nz)), partner):
        pl.semaphore_signal(barrier, inc=1, device_id={'cp': peer}, device_id_type=MESH)

    def by_head(src, dst):
        step = 64

        def widen(i, carry):
            wide[pl.ds(i * step, step)] = src[pl.ds(i * step, step)].astype(jnp.float32)
            return carry
        lax.fori_loop(0, latent // step, widen, 0)
        for h in range(per):
            dst[h] = wide[:, h, :].astype(jnp.bfloat16)

    wait_uk.wait()
    by_head(uk_buf, uk_heads)
    x = x_ref[...]
    cq = jnp.zeros((n_req, q_half), jnp.float32)
    for i in range(blocks):
        wait_dq[i].wait()
        cq += jnp.dot(x[:, i * rows:(i + 1) * rows], big[:, i * q_half:(i + 1) * q_half], preferred_element_type=jnp.float32)
    cq_half[core] = cq.astype(jnp.bfloat16).astype(jnp.float32)
    wo_copy.start()
    pl.semaphore_wait(barrier, nz)
    cq_copy = remote(cq_half.at[core], cq_half.at[core], s_sem.at[0], r_sem.at[0], partner)
    cq_copy.start()
    cq_copy.wait_recv()
    cq = jnp.concatenate([cq_half[0], cq_half[1]], axis=1)
    cq_norm = rms_norm(cq, gq_ref[...]).astype(jnp.bfloat16)
    wait_uq.wait()
    q_full = jnp.dot(cq_norm, wuq_buf[...], preferred_element_type=jnp.float32).astype(jnp.bfloat16)
    for h in range(per):
        q_h = q_full[:, h * (nope_dim + rope_dim):(h + 1) * (nope_dim + rope_dim)]
        q_lat = lax.dot_general(q_h[:, :nope_dim], uk_heads[h], (((1,), (1,)), ((), ())), preferred_element_type=jnp.float32)
        q_rope = rope_rotate(q_h[:, nope_dim:].astype(jnp.float32), cos_ref[...], sin_ref[...])
        q_ref[:, h, :latent] = q_lat.astype(jnp.bfloat16).astype(jnp.float32)
        q_rope = jnp.concatenate([q_rope, jnp.zeros((n_req, LANES - rope_dim), jnp.float32)], axis=1)
        q_ref[:, h, latent:] = q_rope.astype(jnp.bfloat16).astype(jnp.float32)
    q_all[:, pl.ds(me, 1)] = q_ref[...].reshape(n_req, 1, per, latent + LANES)

    def new_entry():
        wait_dkv.wait()
        kv = lax.dot_general(x_ref[...], wdkv_buf[...], (((1,), (1,)), ((), ())), preferred_element_type=jnp.float32)
        c_new = rms_norm(kv[:, :latent], gkv_ref[...]).astype(jnp.bfloat16)
        kr_new = rope_rotate(kv[:, latent:], cos_ref[...], sin_ref[...]).astype(jnp.bfloat16)
        cnew_ref[...] = c_new
        knew_ref[...] = kr_new
        cn_ref[...] = c_new.astype(jnp.float32)
        kn_ref[...] = kr_new.astype(jnp.float32)
        wait_uv.wait()
        by_head(uv_buf, uv_heads)

    def q_copy(r, sem, src_dev, off):
        src = q_ref.at[r] if sem < 4 else q_all.at[r, src_dev]
        return remote(src, q_all.at[r, src_dev], q_send.at[r, sem], q_recv.at[r, src_dev], chip(off))

    def cross_copy(r, slot, src_dev):
        src = q_ref.at[r] if slot == 0 else q_all.at[r, src_dev]
        return remote(src, q_all.at[r, src_dev], q_send_x.at[r, slot], q_recv.at[r, src_dev], partner)

    def arrived(r, src_dev):
        remote(q_all.at[r, src_dev], q_all.at[r, src_dev], q_send.at[r, 0], q_recv.at[r, src_dev], partner).wait_recv()

    def gather_near(r):
        for sem, off in enumerate((2, -2, 1, -1)):
            q_copy(r, sem, me, off).start()
        cross_copy(r, 0, me).start()

    def gather_relay(r):
        for way, side in enumerate((1, -1)):
            src_dev = chip(-2 * side)
            arrived(r, src_dev)

            @pl.when(core == way)
            def _(side=side, src_dev=src_dev):
                q_copy(r, 6, src_dev, 2 * side).start()
            q_copy(r, 4 + way, src_dev, side).start()
            cross_copy(r, 1 + way, src_dev).start()
        for way, side in enumerate((1, -1)):
            arrived(r, chip(side))
            cross_copy(r, 3 + way, chip(side)).start()

    def gather_far(r):
        for slot, off in ((5, 3), (6, -3), (7, 4)):
            arrived(r, chip(off))
            cross_copy(r, slot, chip(off)).start()

    def attend(r):
        def from_partner(d, carry):
            arrived(r, d * 2 + 1 - core)
            return carry
        lax.fori_loop(0, nz, from_partner, 0)
        pltpu.make_async_copy(c_hbm.at[r], c_buf.at[r], c_sem.at[r]).wait()
        pltpu.make_async_copy(k_hbm.at[r], k_buf.at[r], k_sem.at[r]).wait()
        q = q_all[r].reshape(heads, latent + LANES)
        q_lat = q[:, :latent].astype(jnp.bfloat16)
        q_rope = q[:, latent:latent + rope_dim].astype(jnp.bfloat16)
        n = ctx_ref[r]
        base = me * t_dev
        step = 512
        top = jnp.full((heads, LANES), LOWEST, jnp.float32)

        def valid(t0):
            return base + t0 + lax.broadcasted_iota(jnp.int32, (1, step), 1) < n

        for t0 in range(0, t_dev, step):
            s = lax.dot_general(q_lat, c_buf[r, t0:t0 + step, :], (((1,), (1,)), ((), ())), preferred_element_type=jnp.float32)
            s += jnp.dot(q_rope, k_buf[r, :, t0:t0 + step], preferred_element_type=jnp.float32)
            s = jnp.where(valid(t0), s * scale, LOWEST)
            s_buf[:, t0:t0 + step] = s
            for j in range(0, step, LANES):
                top = jnp.maximum(top, s[:, j:j + LANES])
        c_new = cn_ref[pl.ds(r, 1)]
        kr_new = kn_ref[pl.ds(r, 1)]
        s_new = (jnp.sum(q_lat.astype(jnp.float32) * c_new, axis=1, keepdims=True)
                 + jnp.sum(q_rope.astype(jnp.float32) * kr_new, axis=1, keepdims=True)) * scale
        owner = jnp.logical_and(n >= base, n < base + t_dev)
        s_new = jnp.where(owner, s_new, LOWEST)
        m = jnp.maximum(jnp.max(top, axis=1, keepdims=True), s_new)
        w_new = jnp.where(owner, jnp.exp(s_new - m), 0.0)
        mass = jnp.zeros((heads, LANES), jnp.float32)
        acc = w_new.astype(jnp.bfloat16).astype(jnp.float32) * c_new
        for t0 in range(0, t_dev, step):
            w = jnp.where(valid(t0), jnp.exp(s_buf[:, t0:t0 + step] - m), 0.0)
            for j in range(0, step, LANES):
                mass += w[:, j:j + LANES]
            acc += jnp.dot(w.astype(jnp.bfloat16), c_buf[r, t0:t0 + step, :], preferred_element_type=jnp.float32)
        put_block(own, (r,), acc, m, jnp.sum(mass, axis=1, keepdims=True) + w_new)

    def cross_sum(r):
        return remote(own.at[r, :, 1 - core], other.at[r], x_send.at[r], x_recv.at[r], partner)

    def flat(block):
        return block.reshape(-1, latent + LANES)

    def hold_copy(r, sem):
        dest, side, slot, off = ((3, 1, 0, 1), (-3, 0, 0, -1), (-1, 0, 1, 1), (1, 1, 1, -1))[sem]
        return remote(mine.at[r, at(dest)], held.at[r, side, slot], h_send.at[r, sem], h_recv.at[r, side, slot], chip(off))

    def far_copy(r, side):
        return remote(mine.at[r, at(4)], held.at[r, side, 2], h_send.at[r, 4], h_recv.at[r, side, 2], chip(4 * side - 2))

    def relay_copy(r, side):
        return remote(relay.at[r, side], last.at[r, side], f_send.at[r, side], f_recv.at[r, side], chip(4 * side - 2))

    def reduce_pair(r):
        cross_sum(r).wait_recv()
        put_block(mine, (r,), *merge([flat(own[r, :, core]), flat(other[r])], latent))
        for side in range(2):
            @pl.when(core == side)
            def _(side=side):
                far_copy(r, side).start()
        for sem in range(4):
            hold_copy(r, sem).start()

    def reduce_relay(r):
        for side in range(2):
            for slot in range(2):
                remote(mine.at[r, 0], held.at[r, side, slot], h_send.at[r, 0], h_recv.at[r, side, slot], partner).wait_recv()

            @pl.when(core == side)
            def _(side=side):
                far_copy(r, side).wait_recv()
        got = [jnp.concatenate([held[r, 0, slot], held[r, 1, slot]]) for slot in range(3)]
        put_block(relay, (r,), *merge([jnp.concatenate([mine[r, at(-2)], mine[r, at(2)]]), *got], latent))
        for side in range(2):
            relay_copy(r, side).start()

    def finish(r):
        for side in range(2):
            relay_copy(r, side).wait_recv()
        acc, _, mass = merge([mine[r, z], last[r, 0], last[r, 1]], latent)
        o_lat[r] = acc / mass

    lane = lax.broadcasted_iota(jnp.int32, (n_req, per, latent + LANES), 2)
    empty = jnp.where(jnp.logical_and(lane >= latent, lane < latent + LANES // 2), LOWEST, 0.0)
    for side in range(2):
        @pl.when(core != side)
        def _(side=side):
            held[:, side, 2] = empty

    def slot(s, carry):
        def at_slot(delay, body):
            r = s - delay

            @pl.when(jnp.logical_and(r >= 0, r < n_req))
            def _():
                body(r)

        at_slot(FAR_TURN, gather_far)
        at_slot(RELAY_TURN, gather_relay)
        at_slot(turn + 6, finish)
        at_slot(turn + 4, reduce_relay)
        at_slot(turn + 2, reduce_pair)

        def compute(r):
            attend(r)
            cross_sum(r).start()
        at_slot(turn, compute)
        return carry

    def near(r, carry):
        gather_near(r)
        return carry
    lax.fori_loop(0, n_req, near, 0)
    new_entry()
    turn = FAR_TURN + 1
    lax.fori_loop(0, n_req + turn + 6, slot, 0)

    o_heads = []
    for h in range(per):
        o_heads.append(jnp.dot(o_lat[:, h, :].astype(jnp.bfloat16), uv_heads[h], preferred_element_type=jnp.float32).astype(jnp.bfloat16))
    o_heads = jnp.concatenate(o_heads, axis=1)
    wo_copy.wait()
    order = sorted(range(1, nz), key=lambda off: -min(off, nz - off)) + [0]

    def piece_copy(off):
        return remote(part.at[at(off)], got.at[off - 1], a_send.at[off - 1], a_recv.at[off - 1], chip(off))

    for off in order:
        cols = pl.ds(pl.multiple_of(at(off) * width, LANES), width)
        part[at(off)] = jnp.dot(o_heads, big[:, cols], preferred_element_type=jnp.float32)
        if off:
            piece_copy(off).start()
    acc = part[z]
    for off in order[-2::-1]:
        piece_copy(off).wait_recv()
        acc += got[off - 1]
    pair[core] = acc
    swap = remote(pair.at[core], pair.at[core], s_sem.at[1], r_sem.at[1], partner)
    swap.start()
    swap.wait_recv()
    part_cols = lambda piece: pl.ds(pl.multiple_of(piece * width, LANES), width)
    got_all = got.at[nz - 1]
    got_all[...] = pair[0] + pair[1]
    out_ref[:, part_cols(z)] = got_all[...]

    def spread(off):
        return remote(got_all, out_ref.at[:, part_cols(z)], b_send.at[off - 1], b_recv.at[off - 1], chip(off))
    for off in order[:-1]:
        spread(off).start()
    for off in order[-2::-1]:
        spread(off).wait_recv()
    cq_copy.wait_send()
    swap.wait_send()
    for off in order[:-1]:
        piece_copy(off).wait_send()
        spread(off).wait_send()

    def drain(r, carry):
        for sem in range(7):
            q_copy(r, sem, me, 1).wait_send()
        for slot_x in range(nz):
            cross_copy(r, slot_x, me).wait_send()
        cross_sum(r).wait_send()
        for sem in range(4):
            hold_copy(r, sem).wait_send()
        far_copy(r, 0).wait_send()
        for side in range(2):
            relay_copy(r, side).wait_send()
        return carry
    lax.fori_loop(0, n_req, drain, 0)


def decode_group(nz, ctx_len, x, g_q, g_kv, cos_tab, sin_tab, w_dq, w_uq, w_dkv_t, w_uk, w_uv, w_o, cache_c, cache_krt, scale):
    n_req, d_model = x.shape
    _, t_dev, latent = cache_c.shape
    rope_dim = cache_krt.shape[1]
    n_dev = 2 * nz
    _, heads, nope_dim = w_uk.shape
    v_dim = w_uv.shape[2]
    per = heads // n_dev
    width = latent + LANES
    q_lora = w_dq.shape[1]
    rows = per * v_dim
    vmem = pl.BlockSpec(memory_space=pltpu.VMEM)
    hbm = pl.BlockSpec(memory_space=pl.ANY)
    dma = pltpu.SemaphoreType.DMA
    f32, bf16 = jnp.float32, jnp.bfloat16
    return pl.pallas_call(
        functools.partial(decode_kernel, nz, scale),
        out_shape=(jax.ShapeDtypeStruct((n_req, d_model), f32),
                   jax.ShapeDtypeStruct((n_req, latent), bf16),
                   jax.ShapeDtypeStruct((n_req, rope_dim), bf16)),
        in_specs=[pl.BlockSpec(memory_space=pltpu.SMEM)] + [vmem] * 5 + [hbm] * 8,
        out_specs=(vmem, vmem, vmem),
        scratch_shapes=[
            pltpu.VMEM((n_req, t_dev, latent), bf16),
            pltpu.VMEM((n_req, rope_dim, t_dev), bf16),
            pltpu.VMEM((n_req, n_dev, per, width), f32),
            pltpu.VMEM((heads, t_dev), f32),
            pltpu.VMEM((n_req, nz, 2, per, width), f32),
            pltpu.VMEM((n_req, nz, per, width), f32),
            pltpu.VMEM((n_req, nz, per, width), f32),
            pltpu.VMEM((n_req, 2, 3, per, width), f32),
            pltpu.VMEM((n_req, 2, per, width), f32),
            pltpu.VMEM((n_req, 2, per, width), f32),
            pltpu.VMEM((rows, d_model), bf16),
            pltpu.VMEM((q_lora, per * (nope_dim + rope_dim)), bf16),
            pltpu.VMEM((latent + rope_dim, d_model), bf16),
            pltpu.VMEM((latent, per, nope_dim), bf16),
            pltpu.VMEM((latent, per, v_dim), bf16),
            pltpu.VMEM((latent, per, v_dim), f32),
            pltpu.VMEM((per, latent, nope_dim), bf16),
            pltpu.VMEM((per, latent, v_dim), bf16),
            pltpu.VMEM((2, n_req, q_lora // 2), f32),
            pltpu.VMEM((n_req, per, width), f32),
            pltpu.VMEM((n_req, latent), f32),
            pltpu.VMEM((n_req, rope_dim), f32),
            pltpu.VMEM((n_req, per, latent), f32),
            pltpu.VMEM((nz, n_req, d_model // nz), f32),
            pltpu.VMEM((nz, n_req, d_model // nz), f32),
            pltpu.VMEM((2, n_req, d_model // nz), f32),
            dma((n_req,)),
            dma((n_req,)),
            dma((n_req, n_dev)),
            dma((n_req, 7)),
            dma((n_req, nz)),
            dma((n_req,)),
            dma((n_req,)),
            dma((n_req, 5)),
            dma((n_req, 2, 3)),
            dma((n_req, 2)),
            dma((n_req, 2)),
            dma((4 + d_model // rows,)),
            dma((2,)), dma((2,)),
            dma((nz - 1,)), dma((nz - 1,)), dma((nz - 1,)), dma((nz - 1,)),
        ],
        compiler_params=pltpu.CompilerParams(collective_id=0, has_side_effects=True, vmem_limit_bytes=67_000_000),
        name='decode_group',
    )(ctx_len, x, g_q.reshape(1, -1), g_kv.reshape(1, -1), cos_tab, sin_tab, w_dq, w_uq, w_dkv_t, w_uk, w_uv, w_o, cache_c, cache_krt)


def solution(mesh):
    nz = mesh.shape['cp'] // 2

    def decode_step(x, w_dq, g_q, w_uq, w_dkv, g_kv, w_uk, w_uv, w_o, cache_c, cache_kr, ctx_len):
        rope_dim = cache_kr.shape[2]
        scale = (w_uk.shape[2] + rope_dim) ** -0.5
        cos_tab, sin_tab = rope_tables(ctx_len, rope_dim)
        cos_tab = jnp.concatenate([cos_tab, cos_tab], axis=1)
        sin_tab = jnp.concatenate([-sin_tab, sin_tab], axis=1)
        attn_out, c_new, kr_new = decode_group(nz, ctx_len, x, g_q, g_kv, cos_tab, sin_tab, w_dq, w_uq, w_dkv.T, w_uk, w_uv, w_o,
                                               cache_c, cache_kr.transpose(0, 2, 1), scale)
        return (x.astype(jnp.float32) + attn_out).astype(jnp.bfloat16), c_new, kr_new

    spec_rows = P('dp', None)
    spec_cache = P('dp', 'cp', None)
    in_specs = (spec_rows, P(), P(), P(), P(), P(), P(), P(), P(), spec_cache, spec_cache, P('dp'))
    out_specs = (spec_rows, spec_rows, spec_rows)
    return jax.shard_map(decode_step, mesh=mesh, in_specs=in_specs, out_specs=out_specs, check_vma=False)
```

```python
import functools

import jax
import jax.numpy as jnp
from jax import lax
from jax.experimental import pallas as pl
from jax.experimental.pallas import tpu as pltpu
from jax.sharding import PartitionSpec as P

NORM_EPS = 1e-6
ROPE_THETA = 10000.0
LANES = 128
AHEAD = 3
RS_TURN = 3
RELAY_TURN = 2
FAR_TURN = 4
LOWEST = float(jnp.finfo(jnp.float32).min)
MESH = pl.DeviceIdType.MESH


def rms_norm(values, gain_vec):
    mean_sq = jnp.mean(jnp.square(values), axis=-1, keepdims=True)
    return values * lax.rsqrt(mean_sq + NORM_EPS) * gain_vec


def rope_tables(positions, rope_dim):
    half_dim = rope_dim // 2
    lane = jnp.arange(rope_dim)
    inv_freq = ROPE_THETA ** (-2.0 * (lane % half_dim).astype(jnp.float32) / rope_dim)
    angles = positions.astype(jnp.float32)[..., None] * inv_freq
    sines = jnp.sin(angles)
    return jnp.cos(angles), jnp.where(lane < half_dim, -sines, sines)


def rope_rotate(values, cos_tab, sin_tab):
    half_dim = values.shape[-1] // 2
    swapped = jnp.concatenate([values[:, half_dim:], values[:, :half_dim]], axis=-1)
    return values * cos_tab + swapped * sin_tab


def merge(blocks, latent):
    half = LANES // 2
    tops = [block[:, latent:latent + 1] for block in blocks]
    top = functools.reduce(jnp.maximum, tops)
    factors = [jnp.exp(one - top) for one in tops]
    acc = sum(block[:, :latent] * factor for block, factor in zip(blocks, factors))
    mass = sum(block[:, latent + half:latent + half + 1] * factor for block, factor in zip(blocks, factors))
    return acc, top, mass


def put_block(ref, index, acc, top, mass):
    latent = acc.shape[-1]
    rows = acc.shape[0]
    shape = ref.at[index].shape
    half = LANES // 2
    ref[index + (slice(None),) * (len(shape) - 1) + (slice(0, latent),)] = acc.reshape(shape[:-1] + (latent,))
    stats = jnp.where(lax.broadcasted_iota(jnp.int32, (rows, LANES), 1) < half, top, mass)
    ref[index + (slice(None),) * (len(shape) - 1) + (slice(latent, latent + LANES),)] = stats.reshape(shape[:-1] + (LANES,))


def decode_kernel(nz, scale, ctx_ref, x_ref, gq_ref, gkv_ref, cos_ref, sin_ref,
                  wdq_hbm, wuq_hbm, wdkv_hbm, wuk_hbm, wuv_hbm, wo_hbm, c_hbm, k_hbm, out_ref, cnew_ref, knew_ref,
                  c_buf, k_buf, q_all, s_buf, own, other, mine, held, relay, last,
                  big, wuq_buf, wdkv_buf, uk_buf, uv_buf, wide, uk_heads, uv_heads,
                  cq_half, q_ref, rope_ref, cn_ref, kn_ref, o_lat, part, got, pair,
                  c_sem, k_sem, q_recv, q_send, q_send_x, x_send, x_recv, h_send, h_recv, f_send, f_recv,
                  w_sem, s_sem, r_sem, a_send, a_recv, b_send, b_recv):
    n_req, t_dev, latent = c_buf.shape
    rope_dim = k_buf.shape[1]
    per = q_ref.shape[1]
    wide_row = latent + LANES
    q_half = cq_half.shape[2]
    v_dim = uv_heads.shape[2]
    nope_dim = uk_heads.shape[2]
    width = part.shape[2]
    n_dev = 2 * nz
    heads = n_dev * per
    me = lax.axis_index('cp')
    z, core = me // 2, me % 2
    partner = me + 1 - 2 * core
    at = lambda off: lax.rem(z + off + nz, nz)
    chip = lambda off: at(off) * 2 + core

    def remote(src, dst, send, recv, target):
        return pltpu.make_async_remote_copy(src_ref=src, dst_ref=dst, send_sem=send, recv_sem=recv,
                                            device_id={'cp': target}, device_id_type=MESH)

    rows = big.shape[0]
    head0 = pl.multiple_of(me * per, 8)
    weights = [pltpu.make_async_copy(wuk_hbm.at[:, pl.ds(head0, per)], uk_buf, w_sem.at[0])]
    q_cols = pl.ds(pl.multiple_of(core * q_half, LANES), q_half)
    blocks = x_ref.shape[1] // rows
    for i in range(blocks):
        weights.append(pltpu.make_async_copy(wdq_hbm.at[i * rows:(i + 1) * rows, q_cols], big.at[:, i * q_half:(i + 1) * q_half], w_sem.at[4 + i]))
    uq_cols = wuq_buf.shape[1]
    weights.append(pltpu.make_async_copy(wuq_hbm.at[:, pl.ds(pl.multiple_of(me * uq_cols, LANES), uq_cols)], wuq_buf, w_sem.at[1]))
    weights.append(pltpu.make_async_copy(wdkv_hbm, wdkv_buf, w_sem.at[2]))
    weights.append(pltpu.make_async_copy(wuv_hbm.at[:, pl.ds(head0, per)], uv_buf, w_sem.at[3]))
    wait_uk, *wait_dq, wait_uq, wait_dkv, wait_uv = weights
    for copy in weights[:-2]:
        copy.start()
    wo_copy = pltpu.make_async_copy(wo_hbm.at[pl.ds(pl.multiple_of(me * rows, LANES), rows)], big, w_sem.at[4])

    barrier = pltpu.get_barrier_semaphore()
    for peer in (*(chip(off) for off in range(1, nz)), partner):
        pl.semaphore_signal(barrier, inc=1, device_id={'cp': peer}, device_id_type=MESH)

    def by_head(src, dst):
        step = 64

        def widen(i, carry):
            wide[pl.ds(i * step, step)] = src[pl.ds(i * step, step)].astype(jnp.float32)
            return carry
        lax.fori_loop(0, latent // step, widen, 0)
        for h in range(per):
            dst[h] = wide[:, h, :].astype(jnp.bfloat16)

    wait_uk.wait()
    by_head(uk_buf, uk_heads)
    x = x_ref[...]
    cq = jnp.zeros((n_req, q_half), jnp.float32)
    for i in range(blocks):
        wait_dq[i].wait()
        cq += jnp.dot(x[:, i * rows:(i + 1) * rows], big[:, i * q_half:(i + 1) * q_half], preferred_element_type=jnp.float32)
    cq_half[core] = cq.astype(jnp.bfloat16).astype(jnp.float32)
    pl.semaphore_wait(barrier, nz)
    cq_copy = remote(cq_half.at[core], cq_half.at[core], s_sem.at[0], r_sem.at[0], partner)
    cq_copy.start()
    cq_copy.wait_recv()
    cq = jnp.concatenate([cq_half[0], cq_half[1]], axis=1)
    cq_norm = rms_norm(cq, gq_ref[...][None]).astype(jnp.bfloat16)
    wait_uq.wait()
    wait_dkv.start()
    for r in range(n_req):
        pltpu.make_async_copy(c_hbm.at[r], c_buf.at[r], c_sem.at[r]).start()
        pltpu.make_async_copy(k_hbm.at[r], k_buf.at[r], k_sem.at[r]).start()
    wait_uv.start()
    wo_copy.start()
    q_full = jnp.dot(cq_norm, wuq_buf[...], preferred_element_type=jnp.float32).astype(jnp.bfloat16)
    for h in range(per):
        q_h = q_full[:, h * (nope_dim + rope_dim):(h + 1) * (nope_dim + rope_dim)]
        q_lat = lax.dot_general(q_h[:, :nope_dim], uk_heads[h], (((1,), (1,)), ((), ())), preferred_element_type=jnp.float32)
        q_rope = rope_rotate(q_h[:, nope_dim:].astype(jnp.float32), cos_ref[...], sin_ref[...])
        q_ref[1:, h, :] = q_lat.astype(jnp.bfloat16).astype(jnp.float32)
        q_rope = jnp.concatenate([q_rope, jnp.zeros((n_req, LANES - rope_dim), jnp.float32)], axis=1)
        rope_ref[:, h, :] = q_rope.astype(jnp.bfloat16).astype(jnp.float32)
    for r in range(0, n_req, 2):
        both = jnp.concatenate([rope_ref[r, :, :rope_dim], rope_ref[r + 1, :, :rope_dim]], axis=1)
        q_ref[0, :, r * rope_dim:(r + 2) * rope_dim] = both
    q_all[:, pl.ds(me, 1)] = q_ref[...].reshape(n_req + 1, 1, per, latent)

    def new_entry():
        wait_dkv.wait()
        kv = lax.dot_general(x_ref[...], wdkv_buf[...], (((1,), (1,)), ((), ())), preferred_element_type=jnp.float32)
        c_new = rms_norm(kv[:, :latent], gkv_ref[...][None]).astype(jnp.bfloat16)
        kr_new = rope_rotate(kv[:, latent:], cos_ref[...], sin_ref[...]).astype(jnp.bfloat16)
        cnew_ref[...] = c_new
        knew_ref[...] = kr_new
        cn_ref[...] = c_new.astype(jnp.float32)
        kn_ref[...] = kr_new.astype(jnp.float32)

    def q_copy(r, sem, src_dev, off):
        src = q_ref.at[r] if src_dev is me else q_all.at[r, src_dev]
        return remote(src, q_all.at[r, src_dev], q_send.at[r, sem], q_recv.at[r, src_dev], chip(off))

    def cross_copy(r, slot, src_dev):
        src = q_ref.at[r] if slot == 0 else q_all.at[r, src_dev]
        return remote(src, q_all.at[r, src_dev], q_send_x.at[r, slot], q_recv.at[r, src_dev], partner)

    def arrived(r, src_dev):
        remote(q_all.at[r, src_dev], q_all.at[r, src_dev], q_send.at[r, 0], q_recv.at[r, src_dev], partner).wait_recv()

    def gather_near(i, carry):
        for sem, off in enumerate((2, -2, 1, -1)):
            q_copy(i, sem, me, off).start()
        cross_copy(i, 0, me).start()
        return carry

    def gather_later(r):
        @pl.when(r + AHEAD < n_req + 1)
        def _():
            gather_near(r + AHEAD, 0)

    def gather_relay(i):
        for way, side in enumerate((1, -1)):
            src_dev = chip(-2 * side)
            arrived(i, src_dev)

            @pl.when(core == way)
            def _(side=side, src_dev=src_dev):
                q_copy(i, 6, src_dev, 2 * side).start()
            q_copy(i, 4 + way, src_dev, side).start()
            cross_copy(i, 1 + way, src_dev).start()
        for way, side in enumerate((1, -1)):
            arrived(i, chip(side))
            cross_copy(i, 3 + way, chip(side)).start()

    def gather_far(i):
        for slot, off in ((5, 3), (6, -3), (7, 4)):
            arrived(i, chip(off))
            cross_copy(i, slot, chip(off)).start()

    def first_too(body):
        def run(r):
            @pl.when(r == 0)
            def _():
                body(0)
            body(r + 1)
        return run

    def attend(r):
        def from_partner(d, carry):
            arrived(r + 1, d * 2 + 1 - core)
            return carry
        lax.fori_loop(0, nz, from_partner, 0)

        @pl.when(r == 0)
        def _():
            for d in range(nz):
                arrived(0, d * 2 + 1 - core)
        pltpu.make_async_copy(c_hbm.at[r], c_buf.at[r], c_sem.at[r]).wait()
        pltpu.make_async_copy(k_hbm.at[r], k_buf.at[r], k_sem.at[r]).wait()
        q_lat = q_all[r + 1].reshape(heads, latent).astype(jnp.bfloat16)
        pair_cols = pl.ds(pl.multiple_of((r // 2) * LANES, LANES), LANES)
        q_rope = q_all[0, :, :, pair_cols].reshape(heads, LANES)
        q_rope = jnp.where(r % 2 == 0, q_rope[:, :rope_dim], q_rope[:, rope_dim:]).astype(jnp.bfloat16)
        n = ctx_ref[r]
        base = me * t_dev
        step = 512
        top = jnp.full((heads, LANES), LOWEST, jnp.float32)

        def valid(t0):
            return base + t0 + lax.broadcasted_iota(jnp.int32, (1, step), 1) < n

        for t0 in range(0, t_dev, step):
            s = lax.dot_general(q_lat, c_buf[r, t0:t0 + step, :], (((1,), (1,)), ((), ())), preferred_element_type=jnp.float32)
            s += jnp.dot(q_rope, k_buf[r, :, t0:t0 + step], preferred_element_type=jnp.float32)
            s = jnp.where(valid(t0), s * scale, LOWEST)
            s_buf[:, t0:t0 + step] = s
            for j in range(0, step, LANES):
                top = jnp.maximum(top, s[:, j:j + LANES])
        c_new = cn_ref[pl.ds(r, 1)]
        kr_new = kn_ref[pl.ds(r, 1)]
        s_new = (jnp.sum(q_lat.astype(jnp.float32) * c_new, axis=1, keepdims=True)
                 + jnp.sum(q_rope.astype(jnp.float32) * kr_new, axis=1, keepdims=True)) * scale
        owner = jnp.logical_and(n >= base, n < base + t_dev)
        s_new = jnp.where(owner, s_new, LOWEST)
        m = jnp.maximum(jnp.max(top, axis=1, keepdims=True), s_new)
        w_new = jnp.where(owner, jnp.exp(s_new - m), 0.0)
        mass = jnp.zeros((heads, LANES), jnp.float32)
        acc = w_new.astype(jnp.bfloat16).astype(jnp.float32) * c_new
        for t0 in range(0, t_dev, step):
            w = jnp.where(valid(t0), jnp.exp(s_buf[:, t0:t0 + step] - m), 0.0)
            for j in range(0, step, LANES):
                mass += w[:, j:j + LANES]
            acc += jnp.dot(w.astype(jnp.bfloat16), c_buf[r, t0:t0 + step, :], preferred_element_type=jnp.float32)
        put_block(own, (r,), acc, m, jnp.sum(mass, axis=1, keepdims=True) + w_new)

    def cross_sum(r):
        return remote(own.at[r, :, 1 - core], other.at[r], x_send.at[r], x_recv.at[r], partner)

    def flat(block):
        return block.reshape(-1, latent + LANES)

    def hold_copy(r, sem):
        dest, side, slot, off = ((3, 1, 0, 1), (-3, 0, 0, -1), (-1, 0, 1, 1), (1, 1, 1, -1))[sem]
        return remote(mine.at[r, at(dest)], held.at[r, side, slot], h_send.at[r, sem], h_recv.at[r, side, slot], chip(off))

    def far_copy(r, side):
        return remote(mine.at[r, at(4)], held.at[r, side, 2], h_send.at[r, 4], h_recv.at[r, side, 2], chip(4 * side - 2))

    def relay_copy(r, side):
        return remote(relay.at[r, side], last.at[r, side], f_send.at[r, side], f_recv.at[r, side], chip(4 * side - 2))

    def reduce_pair(r):
        cross_sum(r).wait_recv()
        put_block(mine, (r,), *merge([flat(own[r, :, core]), flat(other[r])], latent))
        for side in range(2):
            @pl.when(core == side)
            def _(side=side):
                far_copy(r, side).start()
        for sem in range(4):
            hold_copy(r, sem).start()

    def reduce_relay(r):
        for side in range(2):
            for slot in range(2):
                remote(mine.at[r, 0], held.at[r, side, slot], h_send.at[r, 0], h_recv.at[r, side, slot], partner).wait_recv()

            @pl.when(core == side)
            def _(side=side):
                far_copy(r, side).wait_recv()
        got = [jnp.concatenate([held[r, 0, slot], held[r, 1, slot]]) for slot in range(3)]
        put_block(relay, (r,), *merge([jnp.concatenate([mine[r, at(-2)], mine[r, at(2)]]), *got], latent))
        for side in range(2):
            relay_copy(r, side).start()

    def finish(r):
        for side in range(2):
            relay_copy(r, side).wait_recv()
        acc, _, mass = merge([mine[r, z], last[r, 0], last[r, 1]], latent)
        o_lat[r] = acc / mass

    lane = lax.broadcasted_iota(jnp.int32, (n_req, per, wide_row), 2)
    empty = jnp.where(jnp.logical_and(lane >= latent, lane < latent + LANES // 2), LOWEST, 0.0)
    for side in range(2):
        @pl.when(core != side)
        def _(side=side):
            held[:, side, 2] = empty

    def slot(s, carry):
        def at_slot(delay, body):
            r = s - delay

            @pl.when(jnp.logical_and(r >= 0, r < n_req))
            def _():
                body(r)

        at_slot(FAR_TURN, first_too(gather_far))
        at_slot(RELAY_TURN, first_too(gather_relay))
        at_slot(0, gather_later)
        at_slot(turn + 2 * RS_TURN + 2, finish)
        at_slot(turn + RS_TURN + 2, reduce_relay)
        at_slot(turn + 2, reduce_pair)

        def compute(r):
            attend(r)
            cross_sum(r).start()

            @pl.when(r == n_req - 1)
            def _():
                wait_uv.wait()
                by_head(uv_buf, uv_heads)
        at_slot(turn, compute)
        return carry

    lax.fori_loop(0, AHEAD, gather_near, 0)
    new_entry()
    turn = FAR_TURN + 1
    lax.fori_loop(0, n_req + turn + 2 * RS_TURN + 2, slot, 0)

    o_heads = []
    for h in range(per):
        o_heads.append(jnp.dot(o_lat[:, h, :].astype(jnp.bfloat16), uv_heads[h], preferred_element_type=jnp.float32).astype(jnp.bfloat16))
    o_heads = jnp.concatenate(o_heads, axis=1)
    wo_copy.wait()
    order = sorted(range(1, nz), key=lambda off: -min(off, nz - off)) + [0]

    def piece_copy(off):
        return remote(part.at[at(off)], got.at[off - 1], a_send.at[off - 1], a_recv.at[off - 1], chip(off))

    for off in order:
        cols = pl.ds(pl.multiple_of(at(off) * width, LANES), width)
        part[at(off)] = jnp.dot(o_heads, big[:, cols], preferred_element_type=jnp.float32)
        if off:
            piece_copy(off).start()
    acc = part[z]
    for off in order[-2::-1]:
        piece_copy(off).wait_recv()
        acc += got[off - 1]
    pair[core] = acc
    swap = remote(pair.at[core], pair.at[core], s_sem.at[1], r_sem.at[1], partner)
    swap.start()
    swap.wait_recv()
    part_cols = lambda piece: pl.ds(pl.multiple_of(piece * width, LANES), width)
    got_all = got.at[nz - 1]
    got_all[...] = pair[0] + pair[1]
    out_ref[:, part_cols(z)] = got_all[...]

    def spread(off):
        return remote(got_all, out_ref.at[:, part_cols(z)], b_send.at[off - 1], b_recv.at[off - 1], chip(off))
    for off in order[:-1]:
        spread(off).start()
    for off in order[-2::-1]:
        spread(off).wait_recv()
    cq_copy.wait_send()
    swap.wait_send()
    for off in order[:-1]:
        piece_copy(off).wait_send()
        spread(off).wait_send()

    def drain_q(i, carry):
        for sem in range(7):
            q_copy(i, sem, me, 1).wait_send()
        for slot_x in range(nz):
            cross_copy(i, slot_x, me).wait_send()
        return carry
    lax.fori_loop(0, n_req + 1, drain_q, 0)

    def drain(r, carry):
        cross_sum(r).wait_send()
        for sem in range(4):
            hold_copy(r, sem).wait_send()
        far_copy(r, 0).wait_send()
        for side in range(2):
            relay_copy(r, side).wait_send()
        return carry
    lax.fori_loop(0, n_req, drain, 0)


def decode_group(nz, ctx_len, x, g_q, g_kv, cos_tab, sin_tab, w_dq, w_uq, w_dkv_t, w_uk, w_uv, w_o, cache_c, cache_krt, scale):
    n_req, d_model = x.shape
    _, t_dev, latent = cache_c.shape
    rope_dim = cache_krt.shape[1]
    n_dev = 2 * nz
    _, heads, nope_dim = w_uk.shape
    v_dim = w_uv.shape[2]
    per = heads // n_dev
    width = latent + LANES
    q_lora = w_dq.shape[1]
    rows = per * v_dim
    vmem = pl.BlockSpec(memory_space=pltpu.VMEM)
    hbm = pl.BlockSpec(memory_space=pl.ANY)
    dma = pltpu.SemaphoreType.DMA
    f32, bf16 = jnp.float32, jnp.bfloat16
    return pl.pallas_call(
        functools.partial(decode_kernel, nz, scale),
        out_shape=(jax.ShapeDtypeStruct((n_req, d_model), f32),
                   jax.ShapeDtypeStruct((n_req, latent), bf16),
                   jax.ShapeDtypeStruct((n_req, rope_dim), bf16)),
        in_specs=[pl.BlockSpec(memory_space=pltpu.SMEM)] + [vmem] * 5 + [hbm] * 8,
        out_specs=(vmem, vmem, vmem),
        scratch_shapes=[
            pltpu.VMEM((n_req, t_dev, latent), bf16),
            pltpu.VMEM((n_req, rope_dim, t_dev), bf16),
            pltpu.VMEM((n_req + 1, n_dev, per, latent), f32),
            pltpu.VMEM((heads, t_dev), f32),
            pltpu.VMEM((n_req, nz, 2, per, width), f32),
            pltpu.VMEM((n_req, nz, per, width), f32),
            pltpu.VMEM((n_req, nz, per, width), f32),
            pltpu.VMEM((n_req, 2, 3, per, width), f32),
            pltpu.VMEM((n_req, 2, per, width), f32),
            pltpu.VMEM((n_req, 2, per, width), f32),
            pltpu.VMEM((rows, d_model), bf16),
            pltpu.VMEM((q_lora, per * (nope_dim + rope_dim)), bf16),
            pltpu.VMEM((latent + rope_dim, d_model), bf16),
            pltpu.VMEM((latent, per, nope_dim), bf16),
            pltpu.VMEM((latent, per, v_dim), bf16),
            pltpu.VMEM((latent, per, v_dim), f32),
            pltpu.VMEM((per, latent, nope_dim), bf16),
            pltpu.VMEM((per, latent, v_dim), bf16),
            pltpu.VMEM((2, n_req, q_lora // 2), f32),
            pltpu.VMEM((n_req + 1, per, latent), f32),
            pltpu.VMEM((n_req, per, LANES), f32),
            pltpu.VMEM((n_req, latent), f32),
            pltpu.VMEM((n_req, rope_dim), f32),
            pltpu.VMEM((n_req, per, latent), f32),
            pltpu.VMEM((nz, n_req, d_model // nz), f32),
            pltpu.VMEM((nz, n_req, d_model // nz), f32),
            pltpu.VMEM((2, n_req, d_model // nz), f32),
            dma((n_req,)),
            dma((n_req,)),
            dma((n_req + 1, n_dev)),
            dma((n_req + 1, 7)),
            dma((n_req + 1, nz)),
            dma((n_req,)),
            dma((n_req,)),
            dma((n_req, 5)),
            dma((n_req, 2, 3)),
            dma((n_req, 2)),
            dma((n_req, 2)),
            dma((4 + d_model // rows,)),
            dma((2,)), dma((2,)),
            dma((nz - 1,)), dma((nz - 1,)), dma((nz - 1,)), dma((nz - 1,)),
        ],
        compiler_params=pltpu.CompilerParams(collective_id=0, has_side_effects=True, vmem_limit_bytes=67_000_000),
        name='decode_group',
    )(ctx_len, x, g_q, g_kv, cos_tab, sin_tab, w_dq, w_uq, w_dkv_t, w_uk, w_uv, w_o, cache_c, cache_krt)


def emit_kernel(attn_ref, x_ref, c_ref, k_ref, out_ref, cnew_ref, knew_ref):
    out_ref[...] = (x_ref[...].astype(jnp.float32) + attn_ref[...]).astype(out_ref.dtype)
    cnew_ref[...] = c_ref[...]
    knew_ref[...] = k_ref[...]


def emit(attn_out, x, c_new, kr_new):
    return pl.pallas_call(
        emit_kernel,
        out_shape=tuple(jax.ShapeDtypeStruct(a.shape, x.dtype) for a in (x, c_new, kr_new)),
        name='emit',
    )(attn_out, x, c_new, kr_new)


def solution(mesh):
    nz = mesh.shape['cp'] // 2

    def decode_step(x, w_dq, g_q, w_uq, w_dkv, g_kv, w_uk, w_uv, w_o, cache_c, cache_kr, ctx_len):
        rope_dim = cache_kr.shape[2]
        scale = (w_uk.shape[2] + rope_dim) ** -0.5
        cos_tab, sin_tab = rope_tables(ctx_len, rope_dim)
        attn_out, c_new, kr_new = decode_group(nz, ctx_len, x, g_q, g_kv, cos_tab, sin_tab, w_dq, w_uq, w_dkv.T, w_uk, w_uv, w_o,
                                               cache_c, cache_kr.transpose(0, 2, 1), scale)
        return emit(attn_out, x, c_new, kr_new)

    spec_rows = P('dp', None)
    spec_cache = P('dp', 'cp', None)
    in_specs = (spec_rows, P(), P(), P(), P(), P(), P(), P(), P(), spec_cache, spec_cache, P('dp'))
    out_specs = (spec_rows, spec_rows, spec_rows)
    return jax.shard_map(decode_step, mesh=mesh, in_specs=in_specs, out_specs=out_specs, check_vma=False)
```

```python
import functools

import jax
import jax.numpy as jnp
from jax import lax
from jax.experimental import pallas as pl
from jax.experimental.pallas import tpu as pltpu
from jax.sharding import PartitionSpec as P

NORM_EPS = 1e-6
ROPE_THETA = 10000.0
LANES = 128
AHEAD = 9
RS_TURN = 3
RELAY_TURN = 2
FAR_TURN = 6
LOWEST = float(jnp.finfo(jnp.float32).min)
MESH = pl.DeviceIdType.MESH


def rms_norm(values, gain_vec):
    mean_sq = jnp.mean(jnp.square(values), axis=-1, keepdims=True)
    return values * lax.rsqrt(mean_sq + NORM_EPS) * gain_vec


def rope_tables(positions, rope_dim):
    half_dim = rope_dim // 2
    lane = jnp.arange(rope_dim)
    inv_freq = ROPE_THETA ** (-2.0 * (lane % half_dim).astype(jnp.float32) / rope_dim)
    angles = positions.astype(jnp.float32)[..., None] * inv_freq
    sines = jnp.sin(angles)
    return jnp.cos(angles), jnp.where(lane < half_dim, -sines, sines)


def rope_rotate(values, cos_tab, sin_tab):
    half_dim = values.shape[-1] // 2
    swapped = jnp.concatenate([values[:, half_dim:], values[:, :half_dim]], axis=-1)
    return values * cos_tab + swapped * sin_tab


def merge(blocks, latent):
    half = LANES // 2
    tops = [block[:, latent:latent + 1] for block in blocks]
    top = functools.reduce(jnp.maximum, tops)
    factors = [jnp.exp(one - top) for one in tops]
    acc = sum(block[:, :latent] * factor for block, factor in zip(blocks, factors))
    mass = sum(block[:, latent + half:latent + half + 1] * factor for block, factor in zip(blocks, factors))
    return acc, top, mass


def put_block(ref, index, acc, top, mass):
    latent = acc.shape[-1]
    rows = acc.shape[0]
    shape = ref.at[index].shape
    half = LANES // 2
    ref[index + (slice(None),) * (len(shape) - 1) + (slice(0, latent),)] = acc.reshape(shape[:-1] + (latent,))
    stats = jnp.where(lax.broadcasted_iota(jnp.int32, (rows, LANES), 1) < half, top, mass)
    ref[index + (slice(None),) * (len(shape) - 1) + (slice(latent, latent + LANES),)] = stats.reshape(shape[:-1] + (LANES,))


def decode_kernel(nz, scale, ctx_ref, x_ref, gq_ref, gkv_ref, cos_ref, sin_ref,
                  wdq_hbm, wuq_hbm, wdkv_hbm, wuk_hbm, wuv_hbm, wo_hbm, c_hbm, k_hbm, out_ref, cnew_ref, knew_ref,
                  c_buf, k_buf, q_all, s_buf, own, other, mine, held, relay, last,
                  big, wuq_buf, wdkv_buf, uk_buf, uv_buf, wide, uk_heads, uv_heads,
                  cq_half, q_ref, rope_ref, cn_ref, kn_ref, o_lat, part, got, pair,
                  c_sem, k_sem, q_recv, q_send, q_send_x, x_send, x_recv, h_send, h_recv, f_send, f_recv,
                  w_sem, s_sem, r_sem, a_send, a_recv, b_send, b_recv):
    n_req, t_dev, latent = c_buf.shape
    rope_dim = k_buf.shape[1]
    per = q_ref.shape[1]
    wide_row = latent + LANES
    q_half = cq_half.shape[2]
    v_dim = uv_heads.shape[2]
    nope_dim = uk_heads.shape[2]
    width = part.shape[2]
    n_dev = 2 * nz
    heads = n_dev * per
    me = lax.axis_index('cp')
    z, core = me // 2, me % 2
    partner = me + 1 - 2 * core
    at = lambda off: lax.rem(z + off + nz, nz)
    chip = lambda off: at(off) * 2 + core

    def remote(src, dst, send, recv, target):
        return pltpu.make_async_remote_copy(src_ref=src, dst_ref=dst, send_sem=send, recv_sem=recv,
                                            device_id={'cp': target}, device_id_type=MESH)

    rows = big.shape[0]
    head0 = pl.multiple_of(me * per, 8)
    weights = [pltpu.make_async_copy(wuk_hbm.at[:, pl.ds(head0, per)], uk_buf, w_sem.at[0])]
    q_cols = pl.ds(pl.multiple_of(core * q_half, LANES), q_half)
    blocks = x_ref.shape[1] // rows
    for i in range(blocks):
        weights.append(pltpu.make_async_copy(wdq_hbm.at[i * rows:(i + 1) * rows, q_cols], big.at[:, i * q_half:(i + 1) * q_half], w_sem.at[4 + i]))
    uq_cols = wuq_buf.shape[1]
    weights.append(pltpu.make_async_copy(wuq_hbm.at[:, pl.ds(pl.multiple_of(me * uq_cols, LANES), uq_cols)], wuq_buf, w_sem.at[1]))
    weights.append(pltpu.make_async_copy(wdkv_hbm, wdkv_buf, w_sem.at[2]))
    weights.append(pltpu.make_async_copy(wuv_hbm.at[:, pl.ds(head0, per)], uv_buf, w_sem.at[3]))
    wait_uk, *wait_dq, wait_uq, wait_dkv, wait_uv = weights
    for copy in weights[:-2]:
        copy.start()
    wo_copy = pltpu.make_async_copy(wo_hbm.at[pl.ds(pl.multiple_of(me * rows, LANES), rows)], big, w_sem.at[4])

    barrier = pltpu.get_barrier_semaphore()
    for peer in (*(chip(off) for off in range(1, nz)), partner):
        pl.semaphore_signal(barrier, inc=1, device_id={'cp': peer}, device_id_type=MESH)

    def by_head(src, dst):
        step = 64

        def widen(i, carry):
            wide[pl.ds(i * step, step)] = src[pl.ds(i * step, step)].astype(jnp.float32)
            return carry
        lax.fori_loop(0, latent // step, widen, 0)
        for h in range(per):
            dst[h] = wide[:, h, :].astype(jnp.bfloat16)

    wait_uk.wait()
    by_head(uk_buf, uk_heads)
    x = x_ref[...]
    cq = jnp.zeros((n_req, q_half), jnp.float32)
    for i in range(blocks):
        wait_dq[i].wait()
        cq += jnp.dot(x[:, i * rows:(i + 1) * rows], big[:, i * q_half:(i + 1) * q_half], preferred_element_type=jnp.float32)
    cq_half[core] = cq.astype(jnp.bfloat16).astype(jnp.float32)
    pl.semaphore_wait(barrier, nz)
    cq_copy = remote(cq_half.at[core], cq_half.at[core], s_sem.at[0], r_sem.at[0], partner)
    cq_copy.start()
    cq_copy.wait_recv()
    cq = jnp.concatenate([cq_half[0], cq_half[1]], axis=1)
    cq_norm = rms_norm(cq, gq_ref[...][None]).astype(jnp.bfloat16)
    wait_uq.wait()
    wait_dkv.start()
    for r in range(n_req):
        pltpu.make_async_copy(c_hbm.at[r], c_buf.at[r], c_sem.at[r]).start()
        pltpu.make_async_copy(k_hbm.at[r], k_buf.at[r], k_sem.at[r]).start()
    wait_uv.start()
    wo_copy.start()
    q_full = jnp.dot(cq_norm, wuq_buf[...], preferred_element_type=jnp.float32).astype(jnp.bfloat16)
    for h in range(per):
        q_h = q_full[:, h * (nope_dim + rope_dim):(h + 1) * (nope_dim + rope_dim)]
        q_lat = lax.dot_general(q_h[:, :nope_dim], uk_heads[h], (((1,), (1,)), ((), ())), preferred_element_type=jnp.float32)
        q_rope = rope_rotate(q_h[:, nope_dim:].astype(jnp.float32), cos_ref[...], sin_ref[...])
        q_ref[1:, h, :] = q_lat.astype(jnp.bfloat16).astype(jnp.float32)
        q_rope = jnp.concatenate([q_rope, jnp.zeros((n_req, LANES - rope_dim), jnp.float32)], axis=1)
        rope_ref[:, h, :] = q_rope.astype(jnp.bfloat16).astype(jnp.float32)
    for r in range(0, n_req, 2):
        both = jnp.concatenate([rope_ref[r, :, :rope_dim], rope_ref[r + 1, :, :rope_dim]], axis=1)
        q_ref[0, :, r * rope_dim:(r + 2) * rope_dim] = both
    q_all[:, pl.ds(me, 1)] = q_ref[...].reshape(n_req + 1, 1, per, latent)

    def new_entry():
        wait_dkv.wait()
        kv = lax.dot_general(x_ref[...], wdkv_buf[...], (((1,), (1,)), ((), ())), preferred_element_type=jnp.float32)
        c_new = rms_norm(kv[:, :latent], gkv_ref[...][None]).astype(jnp.bfloat16)
        kr_new = rope_rotate(kv[:, latent:], cos_ref[...], sin_ref[...]).astype(jnp.bfloat16)
        cnew_ref[...] = c_new
        knew_ref[...] = kr_new
        cn_ref[...] = c_new.astype(jnp.float32)
        kn_ref[...] = kr_new.astype(jnp.float32)

    def q_copy(r, sem, src_dev, off):
        src = q_ref.at[r] if src_dev is me else q_all.at[r, src_dev]
        return remote(src, q_all.at[r, src_dev], q_send.at[r, sem], q_recv.at[r, src_dev], chip(off))

    def cross_copy(r, slot, src_dev):
        src = q_ref.at[r] if slot == 0 else q_all.at[r, src_dev]
        return remote(src, q_all.at[r, src_dev], q_send_x.at[r, slot], q_recv.at[r, src_dev], partner)

    def arrived(r, src_dev):
        remote(q_all.at[r, src_dev], q_all.at[r, src_dev], q_send.at[r, 0], q_recv.at[r, src_dev], partner).wait_recv()

    def gather_near(i, carry):
        for sem, off in enumerate((2, -2, 1, -1)):
            q_copy(i, sem, me, off).start()
        cross_copy(i, 0, me).start()
        return carry

    def gather_later(r):
        @pl.when(r + AHEAD < n_req + 1)
        def _():
            gather_near(r + AHEAD, 0)

    def gather_relay(i):
        for way, side in enumerate((1, -1)):
            src_dev = chip(-2 * side)
            arrived(i, src_dev)

            @pl.when(core == way)
            def _(side=side, src_dev=src_dev):
                q_copy(i, 6, src_dev, 2 * side).start()
            q_copy(i, 4 + way, src_dev, side).start()
            cross_copy(i, 1 + way, src_dev).start()
        for way, side in enumerate((1, -1)):
            arrived(i, chip(side))
            cross_copy(i, 3 + way, chip(side)).start()

    def gather_far(i):
        for slot, off in ((5, 3), (6, -3), (7, 4)):
            arrived(i, chip(off))
            cross_copy(i, slot, chip(off)).start()

    def first_too(body):
        def run(r):
            @pl.when(r == 0)
            def _():
                body(0)
            body(r + 1)
        return run

    def attend(r):
        def from_partner(d, carry):
            arrived(r + 1, d * 2 + 1 - core)
            return carry
        lax.fori_loop(0, nz, from_partner, 0)

        @pl.when(r == 0)
        def _():
            for d in range(nz):
                arrived(0, d * 2 + 1 - core)
        pltpu.make_async_copy(c_hbm.at[r], c_buf.at[r], c_sem.at[r]).wait()
        pltpu.make_async_copy(k_hbm.at[r], k_buf.at[r], k_sem.at[r]).wait()
        q_lat = q_all[r + 1].reshape(heads, latent).astype(jnp.bfloat16)
        pair_cols = pl.ds(pl.multiple_of((r // 2) * LANES, LANES), LANES)
        q_rope = q_all[0, :, :, pair_cols].reshape(heads, LANES)
        q_rope = jnp.where(r % 2 == 0, q_rope[:, :rope_dim], q_rope[:, rope_dim:]).astype(jnp.bfloat16)
        n = ctx_ref[r]
        base = me * t_dev
        step = 512
        top = jnp.full((heads, LANES), LOWEST, jnp.float32)

        def valid(t0):
            return base + t0 + lax.broadcasted_iota(jnp.int32, (1, step), 1) < n

        for t0 in range(0, t_dev, step):
            s = lax.dot_general(q_lat, c_buf[r, t0:t0 + step, :], (((1,), (1,)), ((), ())), preferred_element_type=jnp.float32)
            s += jnp.dot(q_rope, k_buf[r, :, t0:t0 + step], preferred_element_type=jnp.float32)
            s = jnp.where(valid(t0), s * scale, LOWEST)
            s_buf[:, t0:t0 + step] = s
            for j in range(0, step, LANES):
                top = jnp.maximum(top, s[:, j:j + LANES])
        c_new = cn_ref[pl.ds(r, 1)]
        kr_new = kn_ref[pl.ds(r, 1)]
        s_new = (jnp.sum(q_lat.astype(jnp.float32) * c_new, axis=1, keepdims=True)
                 + jnp.sum(q_rope.astype(jnp.float32) * kr_new, axis=1, keepdims=True)) * scale
        owner = jnp.logical_and(n >= base, n < base + t_dev)
        s_new = jnp.where(owner, s_new, LOWEST)
        m = jnp.maximum(jnp.max(top, axis=1, keepdims=True), s_new)
        w_new = jnp.where(owner, jnp.exp(s_new - m), 0.0)
        mass = jnp.zeros((heads, LANES), jnp.float32)
        acc = w_new.astype(jnp.bfloat16).astype(jnp.float32) * c_new
        for t0 in range(0, t_dev, step):
            w = jnp.where(valid(t0), jnp.exp(s_buf[:, t0:t0 + step] - m), 0.0)
            for j in range(0, step, LANES):
                mass += w[:, j:j + LANES]
            acc += jnp.dot(w.astype(jnp.bfloat16), c_buf[r, t0:t0 + step, :], preferred_element_type=jnp.float32)
        put_block(own, (r,), acc, m, jnp.sum(mass, axis=1, keepdims=True) + w_new)

    def cross_sum(r):
        return remote(own.at[r, :, 1 - core], other.at[r], x_send.at[r], x_recv.at[r], partner)

    def flat(block):
        return block.reshape(-1, latent + LANES)

    def hold_copy(r, sem):
        dest, side, slot, off = ((3, 1, 0, 1), (-3, 0, 0, -1), (-1, 0, 1, 1), (1, 1, 1, -1))[sem]
        return remote(mine.at[r, at(dest)], held.at[r, side, slot], h_send.at[r, sem], h_recv.at[r, side, slot], chip(off))

    def far_copy(r, side):
        return remote(mine.at[r, at(4)], held.at[r, side, 2], h_send.at[r, 4], h_recv.at[r, side, 2], chip(4 * side - 2))

    def relay_copy(r, side):
        return remote(relay.at[r, side], last.at[r, side], f_send.at[r, side], f_recv.at[r, side], chip(4 * side - 2))

    def reduce_pair(r):
        cross_sum(r).wait_recv()
        put_block(mine, (r,), *merge([flat(own[r, :, core]), flat(other[r])], latent))
        for side in range(2):
            @pl.when(core == side)
            def _(side=side):
                far_copy(r, side).start()
        for sem in range(4):
            hold_copy(r, sem).start()

    def reduce_relay(r):
        for side in range(2):
            for slot in range(2):
                remote(mine.at[r, 0], held.at[r, side, slot], h_send.at[r, 0], h_recv.at[r, side, slot], partner).wait_recv()

            @pl.when(core == side)
            def _(side=side):
                far_copy(r, side).wait_recv()
        got = [jnp.concatenate([held[r, 0, slot], held[r, 1, slot]]) for slot in range(3)]
        put_block(relay, (r,), *merge([jnp.concatenate([mine[r, at(-2)], mine[r, at(2)]]), *got], latent))
        for side in range(2):
            relay_copy(r, side).start()

    def finish(r):
        for side in range(2):
            relay_copy(r, side).wait_recv()
        acc, _, mass = merge([mine[r, z], last[r, 0], last[r, 1]], latent)
        o_lat[r] = acc / mass

    lane = lax.broadcasted_iota(jnp.int32, (n_req, per, wide_row), 2)
    empty = jnp.where(jnp.logical_and(lane >= latent, lane < latent + LANES // 2), LOWEST, 0.0)
    for side in range(2):
        @pl.when(core != side)
        def _(side=side):
            held[:, side, 2] = empty

    def slot(s, carry):
        def at_slot(delay, body):
            r = s - delay

            @pl.when(jnp.logical_and(r >= 0, r < n_req))
            def _():
                body(r)

        at_slot(FAR_TURN, first_too(gather_far))
        at_slot(RELAY_TURN, first_too(gather_relay))
        at_slot(0, gather_later)
        at_slot(turn + 2 * RS_TURN + 2, finish)
        at_slot(turn + RS_TURN + 2, reduce_relay)
        at_slot(turn + 2, reduce_pair)

        def compute(r):
            attend(r)
            cross_sum(r).start()

            @pl.when(r == n_req - 1)
            def _():
                wait_uv.wait()
                by_head(uv_buf, uv_heads)
        at_slot(turn, compute)
        return carry

    lax.fori_loop(0, min(AHEAD, n_req + 1), gather_near, 0)
    new_entry()
    turn = FAR_TURN + 1
    lax.fori_loop(0, n_req + turn + 2 * RS_TURN + 2, slot, 0)

    o_heads = []
    for h in range(per):
        o_heads.append(jnp.dot(o_lat[:, h, :].astype(jnp.bfloat16), uv_heads[h], preferred_element_type=jnp.float32).astype(jnp.bfloat16))
    o_heads = jnp.concatenate(o_heads, axis=1)
    wo_copy.wait()
    order = sorted(range(1, nz), key=lambda off: -min(off, nz - off)) + [0]

    def piece_copy(off):
        return remote(part.at[at(off)], got.at[off - 1], a_send.at[off - 1], a_recv.at[off - 1], chip(off))

    for off in order:
        cols = pl.ds(pl.multiple_of(at(off) * width, LANES), width)
        part[at(off)] = jnp.dot(o_heads, big[:, cols], preferred_element_type=jnp.float32)
        if off:
            piece_copy(off).start()
    acc = part[z]
    for off in order[-2::-1]:
        piece_copy(off).wait_recv()
        acc += got[off - 1]
    pair[core] = acc
    swap = remote(pair.at[core], pair.at[core], s_sem.at[1], r_sem.at[1], partner)
    swap.start()
    swap.wait_recv()
    part_cols = lambda piece: pl.ds(pl.multiple_of(piece * width, LANES), width)
    got_all = got.at[nz - 1]
    got_all[...] = pair[0] + pair[1]
    out_ref[:, part_cols(z)] = got_all[...]

    def spread(off):
        return remote(got_all, out_ref.at[:, part_cols(z)], b_send.at[off - 1], b_recv.at[off - 1], chip(off))
    for off in order[:-1]:
        spread(off).start()
    for off in order[-2::-1]:
        spread(off).wait_recv()
    cq_copy.wait_send()
    swap.wait_send()
    for off in order[:-1]:
        piece_copy(off).wait_send()
        spread(off).wait_send()

    def drain_q(i, carry):
        for sem in range(7):
            q_copy(i, sem, me, 1).wait_send()
        for slot_x in range(nz):
            cross_copy(i, slot_x, me).wait_send()
        return carry
    lax.fori_loop(0, n_req + 1, drain_q, 0)

    def drain(r, carry):
        cross_sum(r).wait_send()
        for sem in range(4):
            hold_copy(r, sem).wait_send()
        far_copy(r, 0).wait_send()
        for side in range(2):
            relay_copy(r, side).wait_send()
        return carry
    lax.fori_loop(0, n_req, drain, 0)


def decode_group(nz, ctx_len, x, g_q, g_kv, cos_tab, sin_tab, w_dq, w_uq, w_dkv_t, w_uk, w_uv, w_o, cache_c, cache_krt, scale):
    n_req, d_model = x.shape
    _, t_dev, latent = cache_c.shape
    rope_dim = cache_krt.shape[1]
    n_dev = 2 * nz
    _, heads, nope_dim = w_uk.shape
    v_dim = w_uv.shape[2]
    per = heads // n_dev
    width = latent + LANES
    q_lora = w_dq.shape[1]
    rows = per * v_dim
    vmem = pl.BlockSpec(memory_space=pltpu.VMEM)
    hbm = pl.BlockSpec(memory_space=pl.ANY)
    dma = pltpu.SemaphoreType.DMA
    f32, bf16 = jnp.float32, jnp.bfloat16
    return pl.pallas_call(
        functools.partial(decode_kernel, nz, scale),
        out_shape=(jax.ShapeDtypeStruct((n_req, d_model), f32),
                   jax.ShapeDtypeStruct((n_req, latent), bf16),
                   jax.ShapeDtypeStruct((n_req, rope_dim), bf16)),
        in_specs=[pl.BlockSpec(memory_space=pltpu.SMEM)] + [vmem] * 5 + [hbm] * 8,
        out_specs=(vmem, vmem, vmem),
        scratch_shapes=[
            pltpu.VMEM((n_req, t_dev, latent), bf16),
            pltpu.VMEM((n_req, rope_dim, t_dev), bf16),
            pltpu.VMEM((n_req + 1, n_dev, per, latent), f32),
            pltpu.VMEM((heads, t_dev), f32),
            pltpu.VMEM((n_req, nz, 2, per, width), f32),
            pltpu.VMEM((n_req, nz, per, width), f32),
            pltpu.VMEM((n_req, nz, per, width), f32),
            pltpu.VMEM((n_req, 2, 3, per, width), f32),
            pltpu.VMEM((n_req, 2, per, width), f32),
            pltpu.VMEM((n_req, 2, per, width), f32),
            pltpu.VMEM((rows, d_model), bf16),
            pltpu.VMEM((q_lora, per * (nope_dim + rope_dim)), bf16),
            pltpu.VMEM((latent + rope_dim, d_model), bf16),
            pltpu.VMEM((latent, per, nope_dim), bf16),
            pltpu.VMEM((latent, per, v_dim), bf16),
            pltpu.VMEM((latent, per, v_dim), f32),
            pltpu.VMEM((per, latent, nope_dim), bf16),
            pltpu.VMEM((per, latent, v_dim), bf16),
            pltpu.VMEM((2, n_req, q_lora // 2), f32),
            pltpu.VMEM((n_req + 1, per, latent), f32),
            pltpu.VMEM((n_req, per, LANES), f32),
            pltpu.VMEM((n_req, latent), f32),
            pltpu.VMEM((n_req, rope_dim), f32),
            pltpu.VMEM((n_req, per, latent), f32),
            pltpu.VMEM((nz, n_req, d_model // nz), f32),
            pltpu.VMEM((nz, n_req, d_model // nz), f32),
            pltpu.VMEM((2, n_req, d_model // nz), f32),
            dma((n_req,)),
            dma((n_req,)),
            dma((n_req + 1, n_dev)),
            dma((n_req + 1, 7)),
            dma((n_req + 1, nz)),
            dma((n_req,)),
            dma((n_req,)),
            dma((n_req, 5)),
            dma((n_req, 2, 3)),
            dma((n_req, 2)),
            dma((n_req, 2)),
            dma((4 + d_model // rows,)),
            dma((2,)), dma((2,)),
            dma((nz - 1,)), dma((nz - 1,)), dma((nz - 1,)), dma((nz - 1,)),
        ],
        compiler_params=pltpu.CompilerParams(collective_id=0, has_side_effects=True, vmem_limit_bytes=67_000_000),
        name='decode_group',
    )(ctx_len, x, g_q, g_kv, cos_tab, sin_tab, w_dq, w_uq, w_dkv_t, w_uk, w_uv, w_o, cache_c, cache_krt)


def emit_kernel(attn_ref, x_ref, c_ref, k_ref, out_ref, cnew_ref, knew_ref):
    out_ref[...] = (x_ref[...].astype(jnp.float32) + attn_ref[...]).astype(out_ref.dtype)
    cnew_ref[...] = c_ref[...]
    knew_ref[...] = k_ref[...]


def emit(attn_out, x, c_new, kr_new):
    return pl.pallas_call(
        emit_kernel,
        out_shape=tuple(jax.ShapeDtypeStruct(a.shape, x.dtype) for a in (x, c_new, kr_new)),
        name='emit',
    )(attn_out, x, c_new, kr_new)


def solution(mesh):
    nz = mesh.shape['cp'] // 2

    def decode_step(x, w_dq, g_q, w_uq, w_dkv, g_kv, w_uk, w_uv, w_o, cache_c, cache_kr, ctx_len):
        rope_dim = cache_kr.shape[2]
        scale = (w_uk.shape[2] + rope_dim) ** -0.5
        cos_tab, sin_tab = rope_tables(ctx_len, rope_dim)
        attn_out, c_new, kr_new = decode_group(nz, ctx_len, x, g_q, g_kv, cos_tab, sin_tab, w_dq, w_uq, w_dkv.T, w_uk, w_uv, w_o,
                                               cache_c, cache_kr.transpose(0, 2, 1), scale)
        return emit(attn_out, x, c_new, kr_new)

    spec_rows = P('dp', None)
    spec_cache = P('dp', 'cp', None)
    in_specs = (spec_rows, P(), P(), P(), P(), P(), P(), P(), P(), spec_cache, spec_cache, P('dp'))
    out_specs = (spec_rows, spec_rows, spec_rows)
    return jax.shard_map(decode_step, mesh=mesh, in_specs=in_specs, out_specs=out_specs, check_vma=False)
```
